16 devices in a mesh: dp: 2 (over y, z), sp: 8 (over x, core).
Axes of the slice: x: 4, y: 2, z: 1, core: 2. Of those that a mesh axis runs over, the one named last changes fastest.
The devices are a block of a 4x4x8 slice.
Arguments:
- hidden: bfloat16 [32, 512, 3072], P('dp', 'sp'), parts along dimension 0
- positions: int32 [1024], P(('dp', 'sp')), parts along dimension 0
- long_factor: float32 [64], replicated
- norm_weight: float32 [3072], replicated
- w_qkv: bfloat16 [3072, 5120], replicated
- w_out: bfloat16 [3072, 3072], replicated
- grad_out: bfloat16 [32, 512, 3072], P('dp', 'sp'), parts along dimension 0
Outputs:
- output 1: bfloat16 [32, 512, 3072], P('dp', 'sp'), parts along dimension 0
- output 2: bfloat16 [32, 512, 3072], P('dp', 'sp'), parts along dimension 0
- output 3: float32 [6144], P('dp'), parts along dimension 0
- output 4: float32 [6144, 5120], P('dp'), parts along dimension 0
- output 5: float32 [6144, 3072], P('dp'), parts along dimension 0
There are 2 independent parts. The reference program is written for one: setup_inputs(seed, part) draws one part's arguments, and reference() takes and returns one part's arrays. A program takes and returns all parts, laid end to end along the dimension named above; an argument that names none is the same for every part.
All inputs are finite; a program needn't handle non-finite values.
Results may differ from the reference program's by a relative error of at most 0.0114191.
Values are sent between devices in bfloat16 or wider.
A program may use at most 768 MiB of HBM per device.

```python
import math
import jax
import jax.numpy as jnp
from jax import lax

BATCH_SIZE = 16
SEQ_LEN = 512
MODEL_DIM = 3072
NUM_HEADS = 24
KV_HEADS = 8
HEAD_DIM = 128

QUERY_DIM = NUM_HEADS * HEAD_DIM
KV_DIM = KV_HEADS * HEAD_DIM
GROUP_SIZE = NUM_HEADS // KV_HEADS
NORM_EPS = 1e-5
ROPE_BASE = 10000.0
ROPE_SCALE = math.sqrt(1.0 + math.log(32.0) / math.log(4096.0))


def setup_inputs(seed: int = 0, part: int = 0) -> dict:
    base_key = jax.random.key(seed)
    part_key = jax.random.fold_in(base_key, part)
    key_hidden, key_grad, key_pos = jax.random.split(part_key, 3)
    shared_key = jax.random.key(seed + 1)
    key_factor, key_norm, key_qkv, key_out = jax.random.split(shared_key, 4)
    hidden = jax.random.normal(key_hidden, (BATCH_SIZE, SEQ_LEN, MODEL_DIM), jnp.float32)
    grad_out = jax.random.normal(key_grad, (BATCH_SIZE, SEQ_LEN, MODEL_DIM), jnp.float32)
    pos_steps = jax.random.randint(key_pos, (SEQ_LEN,), 1, 4)
    positions = (jnp.cumsum(pos_steps) - pos_steps[0]).astype(jnp.int32)
    long_factor = jnp.exp(jax.random.uniform(key_factor, (HEAD_DIM // 2,), jnp.float32, 0.0, math.log(32.0)))
    norm_weight = 1.0 + 0.25 * jax.random.normal(key_norm, (MODEL_DIM,), jnp.float32)
    w_qkv = jax.random.normal(key_qkv, (MODEL_DIM, QUERY_DIM + 2 * KV_DIM), jnp.float32) * MODEL_DIM ** -0.5
    w_out = jax.random.normal(key_out, (QUERY_DIM, MODEL_DIM), jnp.float32) * QUERY_DIM ** -0.5
    return {'hidden': hidden.astype(jnp.bfloat16), 'positions': positions, 'long_factor': long_factor, 'norm_weight': norm_weight, 'w_qkv': w_qkv.astype(jnp.bfloat16), 'w_out': w_out.astype(jnp.bfloat16), 'grad_out': grad_out.astype(jnp.bfloat16)}


def rotate_half(head_vals):
    half_dim = HEAD_DIM // 2
    return jnp.concatenate([-head_vals[..., half_dim:], head_vals[..., :half_dim]], axis=-1)


def rope_tables(positions, long_factor):
    exponents = jnp.arange(0, HEAD_DIM, 2).astype(jnp.float32) / HEAD_DIM
    inv_freq = 1.0 / (long_factor * ROPE_BASE ** exponents)
    angles = positions.astype(jnp.float32)[:, None] * inv_freq[None, :]
    cos_half = jnp.cos(angles) * ROPE_SCALE
    sin_half = jnp.sin(angles) * ROPE_SCALE
    return jnp.concatenate([cos_half, cos_half], axis=-1), jnp.concatenate([sin_half, sin_half], axis=-1)


def apply_rope(head_vals, cos_full, sin_full):
    vals_wide = head_vals.astype(jnp.float32)
    return (vals_wide * cos_full + rotate_half(vals_wide) * sin_full).astype(jnp.bfloat16)


def attend_group(operands):
    query_grp, key_grp, value_grp = operands
    scores = jnp.einsum('bqgd,bkd->bgqk', query_grp.astype(jnp.float32), key_grp.astype(jnp.float32)) * HEAD_DIM ** -0.5
    causal = jnp.arange(SEQ_LEN)[:, None] >= jnp.arange(SEQ_LEN)[None, :]
    attn_probs = jax.nn.softmax(jnp.where(causal, scores, -jnp.inf), axis=-1).astype(jnp.bfloat16)
    return jnp.einsum('bgqk,bkd->bqgd', attn_probs.astype(jnp.float32), value_grp.astype(jnp.float32)).astype(jnp.bfloat16)


def block_forward(hidden_wide, norm_weight, w_qkv, w_out, cos_full, sin_full):
    inv_rms = lax.rsqrt(jnp.mean(hidden_wide * hidden_wide, axis=-1, keepdims=True) + NORM_EPS)
    normed = (hidden_wide * inv_rms * norm_weight).astype(jnp.bfloat16)
    qkv_proj = jnp.einsum('bsd,de->bse', normed.astype(jnp.float32), w_qkv).astype(jnp.bfloat16)
    query_raw = qkv_proj[..., :QUERY_DIM].reshape(BATCH_SIZE, SEQ_LEN, KV_HEADS, GROUP_SIZE, HEAD_DIM)
    key_raw = qkv_proj[..., QUERY_DIM:QUERY_DIM + KV_DIM].reshape(BATCH_SIZE, SEQ_LEN, KV_HEADS, HEAD_DIM)
    value_heads = qkv_proj[..., QUERY_DIM + KV_DIM:].reshape(BATCH_SIZE, SEQ_LEN, KV_HEADS, HEAD_DIM)
    query_rot = apply_rope(query_raw, cos_full[:, None, None, :], sin_full[:, None, None, :])
    key_rot = apply_rope(key_raw, cos_full[:, None, :], sin_full[:, None, :])
    attn_out = lax.map(jax.checkpoint(attend_group), (jnp.moveaxis(query_rot, 2, 0), jnp.moveaxis(key_rot, 2, 0), jnp.moveaxis(value_heads, 2, 0)))
    attn_flat = jnp.moveaxis(attn_out, 0, 2).reshape(BATCH_SIZE, SEQ_LEN, QUERY_DIM)
    mixed_out = jnp.einsum('bse,ed->bsd', attn_flat.astype(jnp.float32), w_out)
    return (hidden_wide + mixed_out).astype(jnp.bfloat16)


def reference(hidden, positions, long_factor, norm_weight, w_qkv, w_out, grad_out):
    cos_full, sin_full = rope_tables(positions, long_factor)

    def forward(hidden_wide, norm_gain, qkv_weight, out_weight):
        return block_forward(hidden_wide, norm_gain, qkv_weight, out_weight, cos_full, sin_full)

    out_hidden, pullback = jax.vjp(forward, hidden.astype(jnp.float32), norm_weight, w_qkv.astype(jnp.float32), w_out.astype(jnp.float32))
    grad_wide, grad_norm, grad_wqkv, grad_wout = pullback(grad_out)
    return out_hidden, grad_wide.astype(jnp.bfloat16), grad_norm, grad_wqkv, grad_wout
```

```python
import functools
import math
import jax
import jax.numpy as jnp
from jax import lax
from jax.experimental import pallas as pl
from jax.experimental.pallas import tpu as pltpu
from jax.sharding import PartitionSpec as P

NORM_EPS = 1e-5
ROPE_BASE = 10000.0
ROPE_SCALE = math.sqrt(1.0 + math.log(32.0) / math.log(4096.0))
F32 = jnp.float32
BF16 = jnp.bfloat16
VMEM_LIMIT = 62 * 1024 * 1024
QB = 128


def rope_tables(positions, long_factor):
    head_dim = 2 * long_factor.shape[0]
    exponents = jnp.arange(0, head_dim, 2).astype(F32) / head_dim
    inv_freq = 1.0 / (long_factor * ROPE_BASE ** exponents)
    angles = positions.astype(F32)[..., None] * inv_freq
    cos_half = jnp.cos(angles) * ROPE_SCALE
    sin_half = jnp.sin(angles) * ROPE_SCALE
    return jnp.concatenate([cos_half, cos_half], axis=-1), jnp.concatenate([-sin_half, sin_half], axis=-1)


def norm_forward(hidden, norm_weight):
    hidden_wide = hidden.astype(F32)
    inv_rms = lax.rsqrt(jnp.mean(hidden_wide * hidden_wide, axis=-1, keepdims=True) + NORM_EPS)
    unit_hidden = hidden_wide * inv_rms
    return hidden_wide, inv_rms, unit_hidden, (unit_hidden * norm_weight).astype(BF16)


def dot_nn(a, b):
    return lax.dot_general(a, b, (((1,), (0,)), ((), ())), preferred_element_type=F32)


def dot_nt(a, b):
    return lax.dot_general(a, b, (((1,), (1,)), ((), ())), preferred_element_type=F32)


def dot_tn(a, b):
    return lax.dot_general(a, b, (((0,), (0,)), ((), ())), preferred_element_type=F32)


def attend_kernel(slots, group, hd, r_ref, dy_ref, wq_ref, wo_ref, cos_ref, sin_ref, o_ref, dqkv_ref,
                  qkv_s, do_s, qs, dos, ks, ps, dss):
    ranks, _, _, tl, dim = r_ref.shape
    seq = ranks * tl
    q_cols = slots * group * hd
    k_cols = slots * hd
    nblk = seq // QB
    rpb = QB // tl
    rows_blk = group * QB
    score_scale = hd ** -0.5
    exp_scale = score_scale * math.log2(math.e)

    r = r_ref[...].reshape(seq, dim)
    qkv_s[...] = dot_nn(r, wq_ref[...]).astype(BF16)
    dy = dy_ref[...].reshape(seq, dim)
    do_s[...] = dot_nn(dy, wo_ref[...]).astype(BF16)

    row_ids = lax.broadcasted_iota(jnp.int32, (rows_blk, QB), 0) % QB
    col_ids = lax.broadcasted_iota(jnp.int32, (rows_blk, QB), 1)
    causal = row_ids >= col_ids

    def rope(vals, rows):
        wide = vals.astype(F32)
        return (wide * cos_ref[rows] + pltpu.roll(wide, hd // 2, 1) * sin_ref[rows]).astype(BF16)

    def rope_back(vals, rows):
        wide = vals.astype(BF16).astype(F32)
        return (wide * cos_ref[rows] - pltpu.roll(wide, hd // 2, 1) * sin_ref[rows]).astype(BF16)

    def one_slot(slot, carry):
        q_at = [pl.ds(pl.multiple_of((slot * group + g) * hd, hd), hd) for g in range(group)]
        k_at = pl.ds(pl.multiple_of(q_cols + slot * hd, hd), hd)
        v_at = pl.ds(pl.multiple_of(q_cols + k_cols + slot * hd, hd), hd)
        ks[...] = rope(qkv_s[:, k_at], pl.ds(0, seq))
        for g in range(group):
            for blk in range(nblk):
                rows = pl.ds(blk * QB, QB)
                dst = pl.ds(blk * rows_blk + g * QB, QB)
                qs[dst] = rope(qkv_s[rows, q_at[g]], rows)
                dos[dst] = do_s[rows, q_at[g]]
        for blk in range(nblk):
            span = (blk + 1) * QB
            rows = pl.ds(blk * rows_blk, rows_blk)
            keys = ks[:span]
            vals = qkv_s[:span, v_at]
            scores = dot_nt(qs[rows], keys)
            diag = jnp.where(causal, scores[:, span - QB:], -jnp.inf)
            scores = diag if blk == 0 else jnp.concatenate([scores[:, :span - QB], diag], axis=1)
            top = jnp.max(scores, axis=1, keepdims=True)
            ex = jnp.exp2((scores - top) * exp_scale)
            probs = ex * (1.0 / jnp.sum(ex, axis=1, keepdims=True))
            low = probs.astype(BF16)
            ps[rows, :span] = low
            outs = dot_nn(low, vals).astype(BF16)
            gp = dot_nt(dos[rows], vals).astype(BF16).astype(F32)
            rdot = jnp.sum(gp * probs, axis=1, keepdims=True)
            gs = (probs * (gp - rdot) * score_scale).astype(BF16)
            dss[rows, :span] = gs
            gq = dot_nn(gs, keys)
            for g in range(group):
                part = outs[g * QB:(g + 1) * QB].reshape(rpb, tl, hd)
                o_ref[blk * rpb:(blk + 1) * rpb, 0, :, q_at[g]] = part
                back = rope_back(gq[g * QB:(g + 1) * QB], pl.ds(blk * QB, QB)).reshape(rpb, tl, hd)
                dqkv_ref[blk * rpb:(blk + 1) * rpb, 0, :, q_at[g]] = back
        for blk in range(nblk):
            rows = pl.ds(blk * rows_blk, (nblk - blk) * rows_blk)
            cols = slice(blk * QB, (blk + 1) * QB)
            gv = dot_tn(ps[rows, cols], dos[rows]).astype(BF16).reshape(rpb, tl, hd)
            gk = rope_back(dot_tn(dss[rows, cols], qs[rows]), pl.ds(blk * QB, QB)).reshape(rpb, tl, hd)
            dqkv_ref[blk * rpb:(blk + 1) * rpb, 0, :, v_at] = gv
            dqkv_ref[blk * rpb:(blk + 1) * rpb, 0, :, k_at] = gk
        return carry

    lax.fori_loop(0, slots, one_slot, 0)


def attend_chunk(gathered, wq_own, wo_own_t, cos_full, sin_full, slots):
    ranks, _, nb, tl, dim = gathered.shape
    seq, hd = cos_full.shape
    q_cols = wo_own_t.shape[1]
    cols = wq_own.shape[1]
    group = q_cols // (slots * hd)
    flops = 2 * nb * seq * dim * (cols + q_cols) + 2 * 6 * nb * slots * group * seq * seq * hd
    token = lambda which: pl.BlockSpec((ranks, 1, 1, tl, dim), lambda b: (0, which, b, 0, 0))
    whole = lambda shape: pl.BlockSpec(shape, lambda b: (0, 0), pipeline_mode=pl.Buffered(1))
    return pl.pallas_call(
        functools.partial(attend_kernel, slots, group, hd),
        grid=(nb,),
        in_specs=[token(0), token(1), whole(wq_own.shape), whole(wo_own_t.shape), whole((seq, hd)), whole((seq, hd))],
        out_specs=[pl.BlockSpec((ranks, 1, tl, q_cols), lambda b: (0, b, 0, 0)),
                   pl.BlockSpec((ranks, 1, tl, cols), lambda b: (0, b, 0, 0))],
        out_shape=[jax.ShapeDtypeStruct((ranks, nb, tl, q_cols), BF16),
                   jax.ShapeDtypeStruct((ranks, nb, tl, cols), BF16)],
        scratch_shapes=[pltpu.VMEM((seq, cols), BF16), pltpu.VMEM((seq, q_cols), BF16),
                        pltpu.VMEM((group * seq, hd), BF16), pltpu.VMEM((group * seq, hd), BF16),
                        pltpu.VMEM((seq, hd), BF16),
                        pltpu.VMEM((group * seq, seq), BF16), pltpu.VMEM((group * seq, seq), BF16)],
        compiler_params=pltpu.CompilerParams(dimension_semantics=("arbitrary",), vmem_limit_bytes=VMEM_LIMIT),
        cost_estimate=pl.CostEstimate(flops=flops, bytes_accessed=2 * nb * seq * (2 * dim + cols + q_cols),
                                      transcendentals=nb * slots * group * seq * seq),
        name="attend",
    )(gathered, gathered, wq_own, wo_own_t, cos_full, sin_full)


def weight_grad_kernel(bounds, which, pieces, n_out, *refs):
    chunks = len(bounds) - 1
    lefts, rights = refs[:chunks], refs[chunks:2 * chunks]
    outs = refs[len(refs) - 4 - n_out:len(refs) - 4]
    lbuf, rbuf, acc, sems = refs[len(refs) - 4:]
    total = bounds[-1]

    def fetch(step, slot, go):
        for c in range(chunks):
            def pair():
                at = step - bounds[c]
                out = []
                for side, (ref, buf, sel) in enumerate(((lefts[c], lbuf, which[0]), (rights[c], rbuf, which[1]))):
                    kind, val, width = sel
                    src = ref.at[:, val, at] if kind == "plane" else ref.at[:, at, :, pl.ds(val, width)]
                    out.append(pltpu.make_async_copy(src, buf.at[slot], sems.at[side, slot]))
                return out
            if go:
                @pl.when((step >= bounds[c]) & (step < bounds[c + 1]))
                def _():
                    for copy in pair():
                        copy.start()
            elif c == 0:
                for side, buf in ((0, lbuf), (1, rbuf)):
                    pltpu.make_async_copy(buf.at[slot], buf.at[slot], sems.at[side, slot]).wait()

    fetch(0, 0, True)
    acc[...] = jnp.zeros_like(acc)

    def body(step, carry):
        slot = lax.rem(step, 2)

        @pl.when(step + 1 < total)
        def _():
            fetch(step + 1, 1 - slot, True)
        fetch(step, slot, False)
        left = lbuf[slot]
        right = rbuf[slot]
        acc[...] += dot_tn(left.reshape(-1, left.shape[-1]), right.reshape(-1, right.shape[-1]))
        return carry

    lax.fori_loop(0, total, body, 0)
    copies = []
    for n, (out, src_rows, src_cols, dst_rows, dst_cols) in enumerate(pieces):
        copy = pltpu.make_async_copy(acc.at[pl.ds(*src_rows), pl.ds(*src_cols)],
                                     outs[out].at[pl.ds(*dst_rows()), pl.ds(*dst_cols())], sems.at[2, n])
        copy.start()
        copies.append(copy)
    for copy in copies:
        copy.wait()


def weight_grad(lefts, rights, which, bounds, acc_shape, pieces, out_structs, carried, name):
    chunks = len(lefts)
    any_spec = pl.BlockSpec(memory_space=pl.ANY)

    def buf(ref, sel):
        return (2, ref.shape[0], ref.shape[-2], ref.shape[-1] if sel[0] == "plane" else sel[2])
    operands = list(lefts) + list(rights) + ([] if carried is None else [carried])
    rows = bounds[-1] * lefts[0].shape[0] * lefts[0].shape[-2]
    return pl.pallas_call(
        functools.partial(weight_grad_kernel, bounds, which, pieces, len(out_structs)),
        in_specs=[any_spec] * len(operands),
        out_specs=[any_spec] * len(out_structs),
        out_shape=out_structs,
        scratch_shapes=[pltpu.VMEM(buf(lefts[0], which[0]), BF16), pltpu.VMEM(buf(rights[0], which[1]), BF16),
                        pltpu.VMEM(acc_shape, F32), pltpu.SemaphoreType.DMA((3, max(2, len(pieces))))],
        input_output_aliases={} if carried is None else {2 * chunks: 0},
        compiler_params=pltpu.CompilerParams(vmem_limit_bytes=VMEM_LIMIT),
        cost_estimate=pl.CostEstimate(flops=2 * rows * acc_shape[0] * acc_shape[1],
                                      bytes_accessed=2 * rows * (acc_shape[0] + acc_shape[1]) + 8 * acc_shape[0] * acc_shape[1],
                                      transcendentals=0),
        name=name,
    )(*operands)


def place_kernel(src_ref, full_ref, out_ref):
    del full_ref
    out_ref[...] = src_ref[...]


def place(full, src, block, grid, src_map, dst_map, name):
    return pl.pallas_call(
        place_kernel,
        grid=grid,
        in_specs=[pl.BlockSpec(block, src_map), pl.BlockSpec(memory_space=pl.ANY)],
        out_specs=pl.BlockSpec(block, dst_map),
        out_shape=jax.ShapeDtypeStruct(full.shape, full.dtype),
        input_output_aliases={1: 0},
        compiler_params=pltpu.CompilerParams(vmem_limit_bytes=VMEM_LIMIT),
        cost_estimate=pl.CostEstimate(flops=src.size, bytes_accessed=8 * src.size, transcendentals=0),
        name=name,
    )(src, full)


def block_body(ranks, hidden, positions, long_factor, norm_weight, w_qkv, w_out, grad_out):
    batch, tl, dim = hidden.shape
    hd = 2 * long_factor.shape[0]
    q_dim = w_out.shape[0]
    kv_dim = (w_qkv.shape[1] - q_dim) // 2
    group = q_dim // kv_dim
    me = lax.axis_index('sp')
    core = lax.rem(me, 2)
    pair = [(i, i ^ 1) for i in range(ranks)]
    qh, kh = q_dim // 2, kv_dim // 2
    slots = kh // hd

    hidden_wide, inv_rms, unit_hidden, normed = norm_forward(hidden, norm_weight)
    sizes = [1, 1] + [2] * ((batch - 2) // 2)
    bounds = [sum(sizes[:i]) for i in range(len(sizes) + 1)]
    both = jnp.stack([normed, grad_out])
    gathered = [lax.all_gather(both[:, bounds[i]:bounds[i + 1]], 'sp') for i in range(len(sizes))]
    pos_all = lax.all_gather(positions, 'sp', tiled=True)
    cos_full, sin_full = rope_tables(pos_all, long_factor)

    wq_own = jnp.concatenate([lax.dynamic_slice_in_dim(w_qkv, core * qh, qh, 1),
                              lax.dynamic_slice_in_dim(w_qkv, q_dim + core * kh, kh, 1),
                              lax.dynamic_slice_in_dim(w_qkv, q_dim + kv_dim + core * kh, kh, 1)], axis=1)
    wo_own_t = lax.dynamic_slice_in_dim(w_out, core * qh, qh, 0).T

    o_parts, g_parts = [], []
    for chunk in gathered:
        o_c, g_c = attend_chunk(chunk, wq_own, wo_own_t, cos_full, sin_full, slots)
        o_parts.append(o_c)
        g_parts.append(g_c)

    def tokens_of(parts, who):
        return jnp.concatenate([lax.dynamic_index_in_dim(p, who, 0, keepdims=False) for p in parts], axis=0)

    other = me + 1 - 2 * core
    o_mine, g_mine = tokens_of(o_parts, me), tokens_of(g_parts, me)
    o_pair = lax.ppermute(tokens_of(o_parts, other), 'sp', pair)
    g_pair = lax.ppermute(tokens_of(g_parts, other), 'sp', pair)

    def in_order(mine, peer, widths):
        lo = jnp.where(core == 0, mine, peer)
        hi = jnp.where(core == 0, peer, mine)
        cols, at = [], 0
        for w in widths:
            cols += [lo[..., at:at + w], hi[..., at:at + w]]
            at += w
        return jnp.concatenate(cols, axis=-1)

    attn_flat = in_order(o_mine, o_pair, [qh])
    grad_qkv = in_order(g_mine, g_pair, [qh, kh, kh])

    half = (qh + 2 * kh) // 2
    q_left = qh - half
    core_id = lambda: lax.rem(lax.axis_index('sp'), 2)
    full_rows = lambda n: (lambda: (0, n))
    at = lambda base, step, width: (lambda: (pl.multiple_of(base + core_id() * step, 128), width))
    full_struct = jax.ShapeDtypeStruct((dim, q_dim + 2 * kv_dim), F32)
    send_struct = jax.ShapeDtypeStruct((dim, half), F32)
    all_rows = (0, dim)
    dwq, send_a = weight_grad(
        gathered, g_parts, (("plane", 0, dim), ("cols", 0, half)), bounds, (dim, half),
        [(0, all_rows, (0, half), full_rows(dim), at(0, qh, half)), (1, all_rows, (0, half), full_rows(dim), full_rows(half))],
        [full_struct, send_struct], None, "wgrad_qkv_a")
    dwq, send_b = weight_grad(
        gathered, g_parts, (("plane", 0, dim), ("cols", half, half)), bounds, (dim, half),
        [(0, all_rows, (0, q_left), full_rows(dim), at(half, qh, q_left)),
         (0, all_rows, (q_left, kh), full_rows(dim), at(q_dim, kh, kh)),
         (0, all_rows, (q_left + kh, kh), full_rows(dim), at(q_dim + kv_dim, kh, kh)),
         (1, all_rows, (0, half), full_rows(dim), full_rows(half))],
        [full_struct, send_struct], dwq, "wgrad_qkv_b")
    dwo, send_o = weight_grad(
        o_parts, gathered, (("cols", 0, qh), ("plane", 1, dim)), bounds, (qh, dim),
        [(0, (0, qh), (0, dim), at(0, qh, qh), full_rows(dim)), (1, (0, qh), (0, dim), full_rows(qh), full_rows(dim))],
        [jax.ShapeDtypeStruct((q_dim, dim), F32), jax.ShapeDtypeStruct((qh, dim), F32)], None, "wgrad_out")
    recv_a = lax.ppermute(send_a, 'sp', pair)
    recv_b = lax.ppermute(send_b, 'sp', pair)
    recv_o = lax.ppermute(send_o, 'sp', pair)

    mixed_out = jnp.einsum('bse,ed->bsd', attn_flat, w_out, preferred_element_type=F32)
    out_hidden = (hidden_wide + mixed_out).astype(BF16)
    grad_normed = jnp.einsum('bse,de->bsd', grad_qkv, w_qkv, preferred_element_type=F32).astype(BF16)
    grad_norm = jnp.sum(grad_normed * unit_hidden, axis=(0, 1))
    grad_unit = grad_normed * norm_weight
    grad_inner = inv_rms * (grad_unit - unit_hidden * jnp.mean(grad_unit * unit_hidden, axis=-1, keepdims=True))
    grad_hidden = (grad_out.astype(F32) + grad_inner).astype(BF16)
    hop = 1
    while hop < ranks:
        grad_norm = grad_norm + lax.ppermute(grad_norm, 'sp', [(i, i ^ hop) for i in range(ranks)])
        hop *= 2

    peer = lambda: 1 - core_id()
    tile = 256
    qt, kt, ht = qh // tile, kh // tile, half // tile
    rows_b = dim // 2

    def place_cols(full, recv, first, name):
        def dst(i, j):
            at_col = first + j
            return i, jnp.where(at_col < qt, peer() * qt + at_col,
                                jnp.where(at_col < qt + kt, q_dim // tile + peer() * kt + at_col - qt,
                                          (q_dim + kv_dim) // tile + peer() * kt + at_col - qt - kt))
        return place(full, recv, (rows_b, tile), (2, ht), lambda i, j: (i, j), dst, name)
    dwq = place_cols(dwq, recv_a, 0, "place_qkv_a")
    dwq = place_cols(dwq, recv_b, ht, "place_qkv_b")
    dwo = place(dwo, recv_o, (tile, dim), (qh // tile,), lambda i: (i, 0), lambda i: (peer() * qt + i, 0), "place_out")
    return out_hidden, grad_hidden, grad_norm, dwq, dwo


def solution(mesh):
    token_spec = P('dp', 'sp', None)
    return jax.shard_map(functools.partial(block_body, mesh.shape['sp']), mesh=mesh,
                         in_specs=(token_spec, P(('dp', 'sp')), P(), P(), P(), P(), token_spec),
                         out_specs=(token_spec, token_spec, P('dp'), P('dp', None), P('dp', None)),
                         check_vma=False)
```

```python
import functools
import math
import jax
import jax.numpy as jnp
from jax import lax
from jax.experimental import pallas as pl
from jax.experimental.pallas import tpu as pltpu
from jax.sharding import PartitionSpec as P

NORM_EPS = 1e-5
ROPE_BASE = 10000.0
ROPE_SCALE = math.sqrt(1.0 + math.log(32.0) / math.log(4096.0))
F32 = jnp.float32
BF16 = jnp.bfloat16
MESH = pl.DeviceIdType.MESH
VMEM_LIMIT = 62 * 1024 * 1024
QB = 128
ANY = pl.BlockSpec(memory_space=pl.ANY)


def dot_nn(a, b):
    return lax.dot_general(a, b, (((1,), (0,)), ((), ())), preferred_element_type=F32)


def dot_nt(a, b):
    return lax.dot_general(a, b, (((1,), (1,)), ((), ())), preferred_element_type=F32)


def dot_tn(a, b):
    return lax.dot_general(a, b, (((0,), (0,)), ((), ())), preferred_element_type=F32)


def lane(index, width):
    return pl.ds(pl.multiple_of(index * width, 128), width)


def my_core():
    return lax.rem(lax.axis_index('sp'), 2)


def half_tables(positions, long_factor):
    half = long_factor.shape[0]
    exponents = jnp.arange(0, 2 * half, 2).astype(F32) / (2 * half)
    inv_freq = 1.0 / (long_factor * ROPE_BASE ** exponents)
    angles = positions.astype(F32)[:, None] * inv_freq
    return jnp.concatenate([jnp.cos(angles) * ROPE_SCALE, jnp.sin(angles) * ROPE_SCALE], axis=-1)


def attend_kernel(ranks, slots, group, hd, nb, rn_ref, dy_ref, wqkv_ref, wout_ref, tab_ref, gath_ref, o_ref, dqkv_ref,
                  wq_s, wo_s, rbuf, dbuf, tabs, cos_s, sin_s, qkv_s, do_s, qs, dos, ks, ps, dss,
                  ssem, rsem, tsend, trecv, wsem, lsem, gsem):
    b = pl.program_id(0)
    tl, dim = rn_ref.shape[1], rn_ref.shape[2]
    seq = ranks * tl
    q_cols, k_cols = slots * group * hd, slots * hd
    q_dim, kv_dim = 2 * q_cols, 2 * k_cols
    me = lax.axis_index('sp')
    core = lax.rem(me, 2)
    peer = me + 1 - 2 * core
    left, right = lax.rem(me + ranks - 2, ranks), lax.rem(me + 2, ranks)
    far = lax.rem(me + 4, ranks)
    cross = 1 - 2 * core

    def rcopy(src, dst, kind, at, target):
        return pltpu.make_async_remote_copy(src_ref=src, dst_ref=dst, send_sem=ssem.at[kind, at],
                                            recv_sem=rsem.at[kind, at], device_id={'sp': target}, device_id_type=MESH)

    def both(rank, at):
        return gath_ref.at[:, rank, at]

    def direct(at):
        for kind, target in ((0, right), (1, left), (4, peer)):
            rcopy(rn_ref.at[at], gath_ref.at[0, me, at], kind, at, target).start()
            rcopy(dy_ref.at[at], gath_ref.at[1, me, at], kind, at, target).start()

    def relay_near(at):
        rcopy(both(left, at), both(left, at), 0, at, me).wait_recv()
        rcopy(both(right, at), both(right, at), 1, at, me).wait_recv()
        rcopy(gath_ref.at[0, left, at], gath_ref.at[0, left, at], 2, at, right).start()
        rcopy(gath_ref.at[1, right, at], gath_ref.at[1, right, at], 3, at, left).start()

    def share_near(at):
        rcopy(both(left, at), both(left, at), 5, at, peer).start()
        rcopy(both(right, at), both(right, at), 6, at, peer).start()

    def relay_far(at):
        rcopy(gath_ref.at[0, far, at], gath_ref.at[0, far, at], 2, at, me).wait_recv()
        rcopy(gath_ref.at[1, far, at], gath_ref.at[1, far, at], 3, at, me).wait_recv()
        rcopy(both(far, at), both(far, at), 7, at, peer).start()

    def wait_shared(at):
        for kind, rank in ((4, peer), (5, left + cross), (6, right + cross), (7, far + cross)):
            rcopy(both(rank, at), both(rank, at), kind, at, me).wait_recv()

    def load(at):
        pltpu.make_async_copy(rn_ref.at[at], rbuf.at[me], lsem.at[0]).start()
        pltpu.make_async_copy(dy_ref.at[at], dbuf.at[me], lsem.at[1]).start()
        for step in range(1, ranks):
            rank = lax.rem(me + step, ranks)
            pltpu.make_async_copy(gath_ref.at[0, rank, at], rbuf.at[rank], lsem.at[0]).start()
            pltpu.make_async_copy(gath_ref.at[1, rank, at], dbuf.at[rank], lsem.at[1]).start()

    def keep_own(at):
        return (pltpu.make_async_copy(rbuf.at[me], gath_ref.at[0, me, at], gsem.at[0]),
                pltpu.make_async_copy(dbuf.at[me], gath_ref.at[1, me, at], gsem.at[1]))

    def table_copy(target):
        return pltpu.make_async_remote_copy(src_ref=tab_ref, dst_ref=tabs.at[me], send_sem=tsend.at[target],
                                            recv_sem=trecv.at[me], device_id={'sp': target}, device_id_type=MESH)

    def weight_copies():
        return (pltpu.make_async_copy(wqkv_ref.at[:, lane(core, q_cols)], wq_s.at[:, pl.ds(0, q_cols)], wsem.at[0]),
                pltpu.make_async_copy(wqkv_ref.at[:, pl.ds(pl.multiple_of(q_dim + core * k_cols, 128), k_cols)],
                                      wq_s.at[:, pl.ds(q_cols, k_cols)], wsem.at[1]),
                pltpu.make_async_copy(wqkv_ref.at[:, pl.ds(pl.multiple_of(q_dim + kv_dim + core * k_cols, 128), k_cols)],
                                      wq_s.at[:, pl.ds(q_cols + k_cols, k_cols)], wsem.at[2]),
                pltpu.make_async_copy(wout_ref.at[pl.ds(pl.multiple_of(core * q_cols, 128), q_cols)], wo_s, wsem.at[3]))

    @pl.when(b == 0)
    def _():
        for copy in weight_copies():
            copy.start()
        own_table = pltpu.make_async_copy(tab_ref, tabs.at[me], wsem.at[4])
        own_table.start()
        barrier = pltpu.get_barrier_semaphore()
        for step in range(1, ranks):
            pl.semaphore_signal(barrier, inc=1, device_id={'sp': lax.rem(me + step, ranks)}, device_id_type=MESH)
        pl.semaphore_wait(barrier, ranks - 1)
        direct(0)
        for step in range(1, ranks):
            table_copy(lax.rem(me + step, ranks)).start()
        relay_near(0)
        direct(1)
        share_near(0)
        own_table.wait()
        for step in range(1, ranks):
            rank = lax.rem(me + step, ranks)
            pltpu.make_async_remote_copy(src_ref=tab_ref, dst_ref=tabs.at[rank], send_sem=tsend.at[rank],
                                         recv_sem=trecv.at[rank], device_id={'sp': rank}, device_id_type=MESH).wait()
        tab = tabs[...].reshape(seq, hd)
        turned = pltpu.roll(tab, hd // 2, 1)
        low = lax.broadcasted_iota(jnp.int32, (seq, hd), 1) < hd // 2
        cos_s[...] = jnp.where(low, tab, turned)
        sin_s[...] = jnp.where(low, -turned, tab)
        relay_far(0)
        wait_shared(0)
        load(0)
        for copy in weight_copies():
            copy.wait()

    @pl.when(b + 1 < nb)
    def _():
        relay_near(b + 1)

    @pl.when(b + 2 < nb)
    def _():
        direct(b + 2)

    @pl.when(b + 1 < nb)
    def _():
        share_near(b + 1)

    pltpu.make_async_copy(rbuf, rbuf, lsem.at[0]).wait()
    pltpu.make_async_copy(dbuf, dbuf, lsem.at[1]).wait()
    for copy in keep_own(b):
        copy.start()
    qkv_s[...] = dot_nn(rbuf[...].reshape(seq, dim), wq_s[...]).astype(BF16)
    do_s[...] = dot_nt(dbuf[...].reshape(seq, dim), wo_s[...]).astype(BF16)

    nblk = seq // QB
    rpb = QB // tl
    rows_blk = group * QB
    score_scale = hd ** -0.5
    exp_scale = score_scale * math.log2(math.e)
    row_ids = lax.broadcasted_iota(jnp.int32, (rows_blk, QB), 0) % QB
    col_ids = lax.broadcasted_iota(jnp.int32, (rows_blk, QB), 1)
    causal = row_ids >= col_ids

    def rope(vals, rows):
        wide = vals.astype(F32)
        return (wide * cos_s[rows] + pltpu.roll(wide, hd // 2, 1) * sin_s[rows]).astype(BF16)

    def rope_back(vals, rows):
        wide = vals.astype(BF16).astype(F32)
        return (wide * cos_s[rows] - pltpu.roll(wide, hd // 2, 1) * sin_s[rows]).astype(BF16)

    def one_slot(slot, carry):
        q_at = [lane(slot * group + g, hd) for g in range(group)]
        k_at = pl.ds(pl.multiple_of(q_cols + slot * hd, hd), hd)
        v_at = pl.ds(pl.multiple_of(q_cols + k_cols + slot * hd, hd), hd)
        ks[...] = rope(qkv_s[:, k_at], pl.ds(0, seq))
        for g in range(group):
            for blk in range(nblk):
                rows = pl.ds(blk * QB, QB)
                dst = pl.ds(blk * rows_blk + g * QB, QB)
                qs[dst] = rope(qkv_s[rows, q_at[g]], rows)
                dos[dst] = do_s[rows, q_at[g]]
        for blk in range(nblk):
            span = (blk + 1) * QB
            rows = pl.ds(blk * rows_blk, rows_blk)
            keys = ks[:span]
            vals = qkv_s[:span, v_at]
            scores = dot_nt(qs[rows], keys)
            diag = jnp.where(causal, scores[:, span - QB:], -jnp.inf)
            scores = diag if blk == 0 else jnp.concatenate([scores[:, :span - QB], diag], axis=1)
            top = jnp.max(scores, axis=1, keepdims=True)
            ex = jnp.exp2((scores - top) * exp_scale)
            probs = ex * (1.0 / jnp.sum(ex, axis=1, keepdims=True))
            low = probs.astype(BF16)
            ps[rows, :span] = low
            outs = dot_nn(low, vals).astype(BF16)
            gp = dot_nt(dos[rows], vals).astype(BF16).astype(F32)
            rdot = jnp.sum(gp * probs, axis=1, keepdims=True)
            gs = (probs * (gp - rdot) * score_scale).astype(BF16)
            dss[rows, :span] = gs
            gq = dot_nn(gs, keys)
            for g in range(group):
                part = outs[g * QB:(g + 1) * QB].reshape(rpb, tl, hd)
                o_ref[blk * rpb:(blk + 1) * rpb, 0, :, q_at[g]] = part
                back = rope_back(gq[g * QB:(g + 1) * QB], pl.ds(blk * QB, QB)).reshape(rpb, tl, hd)
                dqkv_ref[blk * rpb:(blk + 1) * rpb, 0, :, q_at[g]] = back
        for blk in range(nblk):
            rows = pl.ds(blk * rows_blk, (nblk - blk) * rows_blk)
            cols = slice(blk * QB, (blk + 1) * QB)
            gv = dot_tn(ps[rows, cols], dos[rows]).astype(BF16).reshape(rpb, tl, hd)
            gk = rope_back(dot_tn(dss[rows, cols], qs[rows]), pl.ds(blk * QB, QB)).reshape(rpb, tl, hd)
            dqkv_ref[blk * rpb:(blk + 1) * rpb, 0, :, v_at] = gv
            dqkv_ref[blk * rpb:(blk + 1) * rpb, 0, :, k_at] = gk

        @pl.when((slot == 0) & (b + 1 < nb))
        def _():
            relay_far(b + 1)

        @pl.when((slot == 1) & (b + 1 < nb))
        def _():
            for copy in keep_own(b):
                copy.wait()
            wait_shared(b + 1)
            load(b + 1)
        return carry

    lax.fori_loop(0, slots, one_slot, 0)

    @pl.when(b == nb - 1)
    def _():
        for copy in keep_own(b):
            copy.wait()

        def drain(at, carry):
            for kind, rank in ((0, me), (1, me), (4, me), (5, left), (6, right), (7, far)):
                rcopy(both(rank, at), both(rank, at), kind, at, me).wait_send()
            for kind in (2, 3):
                rcopy(gath_ref.at[0, me, at], gath_ref.at[0, me, at], kind, at, me).wait_send()
            return carry
        lax.fori_loop(0, nb, drain, 0)


def attend(normed, grad_out, w_qkv, w_out, table, ranks):
    nb, tl, dim = normed.shape
    hd = table.shape[1]
    seq = ranks * tl
    q_cols, k_cols = w_out.shape[0] // 2, (w_qkv.shape[1] - w_out.shape[0]) // 4
    slots = k_cols // hd
    group = q_cols // k_cols
    cols = q_cols + 2 * k_cols
    flops = 2 * nb * seq * dim * (cols + q_cols) + 2 * 6 * nb * slots * group * seq * seq * hd
    return pl.pallas_call(
        functools.partial(attend_kernel, ranks, slots, group, hd, nb),
        grid=(nb,),
        in_specs=[ANY] * 5,
        out_specs=[ANY, pl.BlockSpec((ranks, 1, tl, q_cols), lambda b: (0, b, 0, 0)),
                   pl.BlockSpec((ranks, 1, tl, cols), lambda b: (0, b, 0, 0))],
        out_shape=[jax.ShapeDtypeStruct((2, ranks, nb, tl, dim), BF16),
                   jax.ShapeDtypeStruct((ranks, nb, tl, q_cols), BF16),
                   jax.ShapeDtypeStruct((ranks, nb, tl, cols), BF16)],
        scratch_shapes=[pltpu.VMEM((dim, cols), BF16), pltpu.VMEM((q_cols, dim), BF16),
                        pltpu.VMEM((ranks, tl, dim), BF16), pltpu.VMEM((ranks, tl, dim), BF16),
                        pltpu.VMEM((ranks, tl, hd), F32), pltpu.VMEM((seq, hd), F32), pltpu.VMEM((seq, hd), F32),
                        pltpu.VMEM((seq, cols), BF16), pltpu.VMEM((seq, q_cols), BF16),
                        pltpu.VMEM((group * seq, hd), BF16), pltpu.VMEM((group * seq, hd), BF16),
                        pltpu.VMEM((seq, hd), BF16),
                        pltpu.VMEM((group * seq, seq), BF16), pltpu.VMEM((group * seq, seq), BF16),
                        pltpu.SemaphoreType.DMA((8, nb)), pltpu.SemaphoreType.DMA((8, nb)),
                        pltpu.SemaphoreType.DMA((ranks,)), pltpu.SemaphoreType.DMA((ranks,)),
                        pltpu.SemaphoreType.DMA((5,)), pltpu.SemaphoreType.DMA((2,)), pltpu.SemaphoreType.DMA((2,))],
        compiler_params=pltpu.CompilerParams(dimension_semantics=("arbitrary",), vmem_limit_bytes=VMEM_LIMIT,
                                             collective_id=0, has_side_effects=True),
        cost_estimate=pl.CostEstimate(flops=flops, bytes_accessed=2 * nb * seq * (4 * dim + cols + q_cols),
                                      transcendentals=nb * slots * group * seq * seq),
        name="attend",
    )(normed, grad_out, w_qkv, w_out, table)


class Placer:
    def __init__(self, recv, full, buf, sems, steps, pieces):
        self.recv, self.full, self.buf, self.sems, self.steps, self.pieces = recv, full, buf, sems, steps, pieces
        self.rows = recv.shape[0] // steps

    def take(self, step):
        at = pl.ds(pl.multiple_of(step * self.rows, 8), self.rows)
        return pltpu.make_async_copy(self.recv.at[at], self.buf.at[lax.rem(step, 2)], self.sems.at[0, lax.rem(step, 2)])

    def put(self, step):
        out = []
        slot = lax.rem(step, 2)
        for n, (src_col, width, dst) in enumerate(self.pieces):
            out.append(pltpu.make_async_copy(self.buf.at[slot, :, pl.ds(src_col, width)], self.full.at[dst(step * self.rows, self.rows, width)],
                                             self.sems.at[1 + n, slot]))
        return out

    def first(self):
        self.take(0).start()

    def step(self, step):
        self.take(step).wait()
        for copy in self.put(step):
            copy.start()

        @pl.when(step >= 1)
        def _():
            for copy in self.put(step - 1):
                copy.wait()

        @pl.when(step + 1 < self.steps)
        def _():
            self.take(step + 1).start()

    def last(self):
        for copy in self.put(self.steps - 1):
            copy.wait()


def peer_cols(base, stride):
    def where(row, rows, width):
        return (pl.ds(pl.multiple_of(row, 8), rows), pl.ds(pl.multiple_of(base + (1 - my_core()) * stride, 128), width))
    return where


def peer_rows(stride):
    def where(row, rows, width):
        return (pl.ds(pl.multiple_of((1 - my_core()) * stride + row, 8), rows), pl.ds(0, width))
    return where


def weight_grad_kernel(total, left_at, right_at, chunks, pieces, place_pieces, n_extra, *refs):
    left_ref, right_ref = refs[0], refs[1]
    n_in = 2 + n_extra
    placing = place_pieces is not None
    n_out = 3 if placing else 2
    outs = refs[n_in:n_in + n_out]
    lbuf, rbuf, acc, sems = refs[n_in + n_out:n_in + n_out + 4]
    placer = None
    if placing:
        placer = Placer(refs[2], outs[2], refs[-2], refs[-1], total, place_pieces)
        placer.first()

    def fetch(step, slot):
        return (pltpu.make_async_copy(left_ref.at[left_at(step)], lbuf.at[slot], sems.at[0, slot]),
                pltpu.make_async_copy(right_ref.at[right_at(step)], rbuf.at[slot], sems.at[1, slot]))

    def flat(buf, slot):
        val = buf[slot]
        return val.reshape(-1, val.shape[-1])

    for copy in fetch(0, 0):
        copy.start()
    acc[...] = jnp.zeros_like(acc)

    def body(step, carry):
        slot = lax.rem(step, 2)
        for copy in fetch(step + 1, 1 - slot):
            copy.start()
        for copy in fetch(step, slot):
            copy.wait()
        if placing:
            placer.step(step)
        acc[...] += dot_tn(flat(lbuf, slot), flat(rbuf, slot))
        return carry

    lax.fori_loop(0, total - 1, body, 0)
    for copy in fetch(total - 1, (total - 1) % 2):
        copy.wait()
    if placing:
        placer.step(jnp.int32(total - 1))
    copies = []
    last = (total - 1) % 2
    part = acc.shape[0] // chunks
    for n in range(chunks):
        rows = pl.ds(n * part, part)
        val = lbuf[last, :, :, n * part:(n + 1) * part]
        acc[rows] += dot_tn(val.reshape(-1, part), flat(rbuf, last))
        for m, (out, src_col, width, dst) in enumerate(pieces):
            copy = pltpu.make_async_copy(acc.at[rows, pl.ds(src_col, width)], outs[out].at[dst(n * part, part, width)],
                                         sems.at[2 + m, n])
            copy.start()
            copies.append(copy)
    for copy in copies:
        copy.wait()
    if placing:
        placer.last()


def weight_grad(left, right, left_sel, right_sel, acc_shape, chunks, pieces, full_struct, carried, place, order, name):
    ranks, nb, tl = right.shape[-4], right.shape[-3], right.shape[-2]

    def at(sel, ref):
        if sel[0] == "plane":
            return (lambda step: (sel[1], slice(None), step)), ref.shape[-1]
        return (lambda step: (slice(None), step, slice(None), pl.ds(sel[1], sel[2]))), sel[2]
    left_at, left_width = at(left_sel, left)
    right_at, right_width = at(right_sel, right)
    operands, aliases = [left, right], {}
    out_shape = [full_struct, jax.ShapeDtypeStruct(acc_shape, F32)]
    scratch = [pltpu.VMEM((2, ranks, tl, left_width), BF16), pltpu.VMEM((2, ranks, tl, right_width), BF16),
               pltpu.VMEM(acc_shape, F32), pltpu.SemaphoreType.DMA((2 + len(pieces), max(2, chunks)))]
    place_pieces = None
    if place is not None:
        recv, full, place_pieces = place
        operands += [recv, full]
        aliases[3] = 2
        out_shape.append(jax.ShapeDtypeStruct(full.shape, F32))
        scratch += [pltpu.VMEM((2, recv.shape[0] // nb, recv.shape[1]), F32),
                    pltpu.SemaphoreType.DMA((1 + len(place_pieces), 2))]
    if carried is not None:
        aliases[len(operands)] = 0
        operands.append(carried)
    operands += order
    rows = ranks * nb * tl
    return pl.pallas_call(
        functools.partial(weight_grad_kernel, nb, left_at, right_at, chunks, pieces, place_pieces, len(operands) - 2),
        in_specs=[ANY] * len(operands),
        out_specs=[ANY] * len(out_shape),
        out_shape=out_shape,
        scratch_shapes=scratch,
        input_output_aliases=aliases,
        compiler_params=pltpu.CompilerParams(vmem_limit_bytes=VMEM_LIMIT),
        cost_estimate=pl.CostEstimate(flops=2 * rows * acc_shape[0] * acc_shape[1],
                                      bytes_accessed=2 * rows * (left_width + right_width) + 8 * acc_shape[0] * acc_shape[1],
                                      transcendentals=0),
        name=name,
    )(*operands)


def canonical_copies(mine_ref, pair_ref, full, sems, parts):
    core, me = my_core(), lax.axis_index('sp')
    out, src, base = [], 0, 0
    for n, width in enumerate(parts):
        for side, ref in enumerate((mine_ref.at[me], pair_ref)):
            owner = core if side == 0 else 1 - core
            dst = pl.ds(pl.multiple_of(base + owner * width, 128), width)
            out.append(pltpu.make_async_copy(ref.at[:, :, pl.ds(src, width)], full.at[:, :, dst], sems.at[n, side]))
        src += width
        base += 2 * width
    return out


def hidden_grad_kernel(parts, place_pieces, w_ref, x_ref, inv_ref, gain_ref, gm_ref, gp_ref, dy_ref, recv_ref, full_in,
                       dx_ref, dg_ref, full_ref, gfull, dn_s, dys, mean_s, bounce, csem, psem, dsem):
    del full_in
    step = pl.program_id(0)
    steps = pl.num_programs(0)
    nb, tl, dim = dys.shape
    rows = nb * tl
    width = w_ref.shape[0]
    placer = Placer(recv_ref, full_ref, bounce, psem, recv_ref.shape[0] // bounce.shape[1], place_pieces)

    @pl.when(step == 0)
    def _():
        for copy in canonical_copies(gm_ref, gp_ref, gfull, csem, parts):
            copy.start()
        placer.first()
        pltpu.make_async_copy(dy_ref, dys, dsem.at[0]).start()
        mean_s[...] = jnp.zeros_like(mean_s)
        for copy in canonical_copies(gm_ref, gp_ref, gfull, csem, parts):
            copy.wait()

    placer.step(step)
    low = dot_nt(gfull[...].reshape(rows, gfull.shape[-1]), w_ref[...]).astype(BF16)
    at = lane(step, width)
    dn_s[:, at] = low
    grad = low.astype(F32)
    unit = x_ref[:, :, at].reshape(rows, width).astype(F32) * inv_ref[...]
    mean_s[...] += jnp.sum(grad * gain_ref[:, at] * unit, axis=1, keepdims=True)
    dg_ref[:, at] = jnp.sum(grad * unit, axis=0, keepdims=True)

    @pl.when(step == steps - 1)
    def _():
        pltpu.make_async_copy(dy_ref, dys, dsem.at[0]).wait()

        def finish(i, carry):
            span = pl.ds(pl.multiple_of(i * tl, tl), tl)
            inv = inv_ref[span]
            unit_rows = x_ref[i].astype(F32) * inv
            inner = inv * (dn_s[span].astype(F32) * gain_ref[...] - unit_rows * (mean_s[span] * (1.0 / dim)))
            dys[i] = (dys[i].astype(F32) + inner).astype(BF16)
            pltpu.make_async_copy(dys.at[i], dx_ref.at[i], dsem.at[1]).start()
            return carry
        lax.fori_loop(0, nb, finish, 0)
        placer.last()
        pltpu.make_async_copy(dys, dx_ref, dsem.at[1]).wait()


def hidden_grad(hidden, grad_out, inv_rms, norm_weight, w_qkv, g_all, g_pair, recv, full, parts, place_pieces):
    nb, tl, dim = hidden.shape
    cols = w_qkv.shape[1]
    width = 512
    steps = dim // width
    const = lambda *shape: pl.BlockSpec(shape, lambda n: (0,) * len(shape), pipeline_mode=pl.Buffered(1))
    return pl.pallas_call(
        functools.partial(hidden_grad_kernel, parts, place_pieces),
        grid=(steps,),
        in_specs=[pl.BlockSpec((width, cols), lambda n: (n, 0)), const(nb, tl, dim), const(nb * tl, 1), const(1, dim),
                  ANY, ANY, ANY, ANY, ANY],
        out_specs=[ANY, const(1, dim), ANY],
        out_shape=[jax.ShapeDtypeStruct((nb, tl, dim), BF16), jax.ShapeDtypeStruct((1, dim), F32),
                   jax.ShapeDtypeStruct(full.shape, F32)],
        scratch_shapes=[pltpu.VMEM((nb, tl, cols), BF16), pltpu.VMEM((nb * tl, dim), BF16), pltpu.VMEM((nb, tl, dim), BF16),
                        pltpu.VMEM((nb * tl, 1), F32), pltpu.VMEM((2, recv.shape[0] // steps, recv.shape[1]), F32),
                        pltpu.SemaphoreType.DMA((len(parts), 2)), pltpu.SemaphoreType.DMA((1 + len(place_pieces), 2)),
                        pltpu.SemaphoreType.DMA((2,))],
        input_output_aliases={8: 2},
        compiler_params=pltpu.CompilerParams(dimension_semantics=("arbitrary",), vmem_limit_bytes=VMEM_LIMIT),
        cost_estimate=pl.CostEstimate(flops=2 * nb * tl * dim * cols, bytes_accessed=2 * dim * cols + 8 * recv.size,
                                      transcendentals=0),
        name="hidden_grad",
    )(w_qkv, hidden, inv_rms, norm_weight, g_all, g_pair, grad_out, recv, full)


def project_out_kernel(parts, place_pieces, w_ref, x_ref, om_ref, op_ref, recv_ref, full_in, y_ref, full_ref,
                       ofull, bounce, csem, psem):
    del full_in
    step = pl.program_id(0)
    steps = pl.num_programs(0)
    nb, tl, q_dim = ofull.shape
    placer = Placer(recv_ref, full_ref, bounce, psem, recv_ref.shape[0] // bounce.shape[1], place_pieces)

    @pl.when(step == 0)
    def _():
        for copy in canonical_copies(om_ref, op_ref, ofull, csem, parts):
            copy.start()
        placer.first()
        for copy in canonical_copies(om_ref, op_ref, ofull, csem, parts):
            copy.wait()

    placer.step(step)
    mixed = dot_nn(ofull[...].reshape(nb * tl, q_dim), w_ref[...])
    y_ref[...] = (x_ref[...].astype(F32) + mixed.reshape(y_ref.shape)).astype(BF16)

    @pl.when(step == steps - 1)
    def _():
        placer.last()


def project_out(hidden, w_out, o_all, o_pair, recv, full, parts, place_pieces):
    nb, tl, dim = hidden.shape
    q_dim = w_out.shape[0]
    width = 512
    steps = dim // width
    tile = pl.BlockSpec((nb, tl, width), lambda n: (0, 0, n))
    return pl.pallas_call(
        functools.partial(project_out_kernel, parts, place_pieces),
        grid=(steps,),
        in_specs=[pl.BlockSpec((q_dim, width), lambda n: (0, n)), tile, ANY, ANY, ANY, ANY],
        out_specs=[tile, ANY],
        out_shape=[jax.ShapeDtypeStruct((nb, tl, dim), BF16), jax.ShapeDtypeStruct(full.shape, F32)],
        scratch_shapes=[pltpu.VMEM((nb, tl, q_dim), BF16), pltpu.VMEM((2, recv.shape[0] // steps, recv.shape[1]), F32),
                        pltpu.SemaphoreType.DMA((len(parts), 2)), pltpu.SemaphoreType.DMA((1 + len(place_pieces), 2))],
        input_output_aliases={5: 1},
        compiler_params=pltpu.CompilerParams(dimension_semantics=("arbitrary",), vmem_limit_bytes=VMEM_LIMIT),
        cost_estimate=pl.CostEstimate(flops=2 * nb * tl * dim * q_dim, bytes_accessed=2 * dim * q_dim + 8 * recv.size,
                                      transcendentals=0),
        name="project_out",
    )(w_out, hidden, o_all, o_pair, recv, full)


def group_sum_kernel(ranks, part_ref, sum_ref, parts, ssem, rsem):
    me = lax.axis_index('sp')
    barrier = pltpu.get_barrier_semaphore()
    for step in range(1, ranks):
        pl.semaphore_signal(barrier, inc=1, device_id={'sp': lax.rem(me + step, ranks)}, device_id_type=MESH)
    pl.semaphore_wait(barrier, ranks - 1)

    def copy(slot, target):
        return pltpu.make_async_remote_copy(src_ref=part_ref, dst_ref=parts.at[slot], send_sem=ssem.at[target],
                                            recv_sem=rsem.at[slot], device_id={'sp': target}, device_id_type=MESH)
    own = pltpu.make_async_copy(part_ref, parts.at[me], ssem.at[me])
    own.start()
    for step in range(1, ranks):
        copy(me, lax.rem(me + step, ranks)).start()
    own.wait()
    for step in range(1, ranks):
        rank = lax.rem(me + step, ranks)
        copy(rank, rank).wait()
    total = parts[0]
    for rank in range(1, ranks):
        total = total + parts[rank]
    sum_ref[...] = total


def group_sum(part, ranks):
    return pl.pallas_call(
        functools.partial(group_sum_kernel, ranks),
        in_specs=[ANY],
        out_specs=pl.BlockSpec(memory_space=pltpu.VMEM),
        out_shape=jax.ShapeDtypeStruct(part.shape, F32),
        scratch_shapes=[pltpu.VMEM((ranks,) + part.shape, F32), pltpu.SemaphoreType.DMA((ranks,)),
                        pltpu.SemaphoreType.DMA((ranks,))],
        compiler_params=pltpu.CompilerParams(collective_id=1, has_side_effects=True),
        cost_estimate=pl.CostEstimate(flops=ranks * part.size, bytes_accessed=8 * ranks * part.size, transcendentals=0),
        name="group_sum",
    )(part)


def block_body(ranks, hidden, positions, long_factor, norm_weight, w_qkv, w_out, grad_out):
    nb, tl, dim = hidden.shape
    hd = 2 * long_factor.shape[0]
    q_dim = w_out.shape[0]
    kv_dim = (w_qkv.shape[1] - q_dim) // 2
    me = lax.axis_index('sp')
    other = me + 1 - 2 * lax.rem(me, 2)
    pair = [(i, i ^ 1) for i in range(ranks)]
    qh, kh = q_dim // 2, kv_dim // 2

    hidden_wide = hidden.astype(F32)
    inv_rms = lax.rsqrt(jnp.mean(hidden_wide * hidden_wide, axis=-1, keepdims=True) + NORM_EPS)
    normed = (hidden_wide * inv_rms * norm_weight).astype(BF16)
    gathered, o_all, g_all = attend(normed, grad_out, w_qkv, w_out, half_tables(positions, long_factor), ranks)
    o_pair = lax.ppermute(lax.dynamic_index_in_dim(o_all, other, 0, keepdims=False), 'sp', pair)
    g_pair = lax.ppermute(lax.dynamic_index_in_dim(g_all, other, 0, keepdims=False), 'sp', pair)

    half = (qh + 2 * kh) // 2
    q_left = qh - half
    dwq_struct = jax.ShapeDtypeStruct(w_qkv.shape, F32)
    dwo_struct = jax.ShapeDtypeStruct(w_out.shape, F32)

    def own_cols(base, stride):
        def where(row, rows, width):
            return (pl.ds(row, rows), pl.ds(pl.multiple_of(base + my_core() * stride, 128), width))
        return where

    def own_rows(stride):
        def where(row, rows, width):
            return (pl.ds(pl.multiple_of(my_core() * stride + row, 8), rows), pl.ds(0, width))
        return where

    def same(row, rows, width):
        return (pl.ds(row, rows), pl.ds(0, width))

    dwo, send_o = weight_grad(o_all, gathered, ("cols", 0, qh), ("plane", 1), (qh, dim), 4,
                              [(0, 0, dim, own_rows(qh)), (1, 0, dim, same)], dwo_struct, None, None, [], "wgrad_out")
    recv_o = lax.ppermute(send_o, 'sp', pair)
    dwq, send_a = weight_grad(gathered, g_all, ("plane", 0), ("cols", 0, half), (dim, half), 4,
                              [(0, 0, half, own_cols(0, qh)), (1, 0, half, same)], dwq_struct, None, None, [dwo],
                              "wgrad_qkv_a")
    recv_a = lax.ppermute(send_a, 'sp', pair)
    dwq, send_b, dwo = weight_grad(gathered, g_all, ("plane", 0), ("cols", half, half), (dim, half), 4,
                                   [(0, 0, q_left, own_cols(half, qh)), (0, q_left, kh, own_cols(q_dim, kh)),
                                    (0, q_left + kh, kh, own_cols(q_dim + kv_dim, kh)), (1, 0, half, same)],
                                   dwq_struct, dwq, (recv_o, dwo, [(0, dim, peer_rows(qh))]), [o_pair, g_pair], "wgrad_qkv_b")
    recv_b = lax.ppermute(send_b, 'sp', pair)
    grad_hidden, grad_norm, dwq = hidden_grad(
        hidden, grad_out, inv_rms.reshape(nb * tl, 1), norm_weight[None], w_qkv, g_all, g_pair, recv_a, dwq,
        [qh, kh, kh], [(0, half, peer_cols(0, qh))])
    out_hidden, dwq = project_out(
        hidden, w_out, o_all, o_pair, recv_b, dwq, [qh],
        [(0, q_left, peer_cols(half, qh)), (q_left, kh, peer_cols(q_dim, kh)), (q_left + kh, kh, peer_cols(q_dim + kv_dim, kh))])
    grad_norm = group_sum(grad_norm.reshape(-1, 128), ranks).reshape(-1)
    return out_hidden, grad_hidden, grad_norm, dwq, dwo


def solution(mesh):
    token_spec = P('dp', 'sp', None)
    return jax.shard_map(functools.partial(block_body, mesh.shape['sp']), mesh=mesh,
                         in_specs=(token_spec, P(('dp', 'sp')), P(), P(), P(), P(), token_spec),
                         out_specs=(token_spec, token_spec, P('dp'), P('dp', None), P('dp', None)),
                         check_vma=False)
```

```python
import functools
import math
import jax
import jax.numpy as jnp
from jax import lax
from jax.experimental import pallas as pl
from jax.experimental.pallas import tpu as pltpu
from jax.sharding import PartitionSpec as P

NORM_EPS = 1e-5
ROPE_BASE = 10000.0
ROPE_SCALE = math.sqrt(1.0 + math.log(32.0) / math.log(4096.0))
F32 = jnp.float32
BF16 = jnp.bfloat16
MESH = pl.DeviceIdType.MESH
VMEM_LIMIT = 67000000
QB = 128
ANY = pl.BlockSpec(memory_space=pl.ANY)


def dot_nn(a, b):
    return lax.dot_general(a, b, (((1,), (0,)), ((), ())), preferred_element_type=F32)


def dot_nt(a, b):
    return lax.dot_general(a, b, (((1,), (1,)), ((), ())), preferred_element_type=F32)


def dot_tn(a, b):
    return lax.dot_general(a, b, (((0,), (0,)), ((), ())), preferred_element_type=F32)


def lane(index, width):
    return pl.ds(pl.multiple_of(index * width, 128), width)


def my_core():
    return lax.rem(lax.axis_index('sp'), 2)


def half_tables(positions, long_factor):
    half = long_factor.shape[0]
    exponents = jnp.arange(0, 2 * half, 2).astype(F32) / (2 * half)
    inv_freq = 1.0 / (long_factor * ROPE_BASE ** exponents)
    angles = positions.astype(F32)[:, None] * inv_freq
    return jnp.concatenate([jnp.cos(angles) * ROPE_SCALE, jnp.sin(angles) * ROPE_SCALE], axis=-1)


def attend_kernel(ranks, slots, group, hd, nb, rn_ref, dy_ref, wqkv_ref, wout_ref, tab_ref, gath_ref, o_ref, dqkv_ref, osend_ref, gsend_ref,
                  wq_s, wo_s, rbuf, dbuf, tabs, cos_s, sin_s, qkv_s, do_s, qs, dos, ks, ps, dss, sc, gps,
                  ssem, rsem, tsend, trecv, wsem, lsem, gsem):
    b = pl.program_id(0)
    tl, dim = rn_ref.shape[1], rn_ref.shape[2]
    seq = ranks * tl
    q_cols, k_cols = slots * group * hd, slots * hd
    q_dim, kv_dim = 2 * q_cols, 2 * k_cols
    me = lax.axis_index('sp')
    core = lax.rem(me, 2)
    peer = me + 1 - 2 * core
    left, right = lax.rem(me + ranks - 2, ranks), lax.rem(me + 2, ranks)
    far = lax.rem(me + 4, ranks)
    cross = 1 - 2 * core

    def rcopy(src, dst, kind, at, target):
        return pltpu.make_async_remote_copy(src_ref=src, dst_ref=dst, send_sem=ssem.at[kind, at],
                                            recv_sem=rsem.at[kind, at], device_id={'sp': target}, device_id_type=MESH)

    def both(rank, at):
        return gath_ref.at[:, rank, at]

    def direct(at):
        for kind, target in ((0, right), (1, left), (4, peer)):
            rcopy(rn_ref.at[at], gath_ref.at[0, me, at], kind, at, target).start()
            rcopy(dy_ref.at[at], gath_ref.at[1, me, at], kind, at, target).start()

    def relay_near(at):
        rcopy(both(left, at), both(left, at), 0, at, me).wait_recv()
        rcopy(both(right, at), both(right, at), 1, at, me).wait_recv()
        rcopy(gath_ref.at[0, left, at], gath_ref.at[0, left, at], 2, at, right).start()
        rcopy(gath_ref.at[1, right, at], gath_ref.at[1, right, at], 3, at, left).start()

    def share_near(at):
        rcopy(both(left, at), both(left, at), 5, at, peer).start()
        rcopy(both(right, at), both(right, at), 6, at, peer).start()

    def relay_far(at):
        rcopy(gath_ref.at[0, far, at], gath_ref.at[0, far, at], 2, at, me).wait_recv()
        rcopy(gath_ref.at[1, far, at], gath_ref.at[1, far, at], 3, at, me).wait_recv()
        rcopy(both(far, at), both(far, at), 7, at, peer).start()

    def wait_shared(at):
        for kind, rank in ((4, peer), (5, left + cross), (6, right + cross), (7, far + cross)):
            rcopy(both(rank, at), both(rank, at), kind, at, me).wait_recv()

    def load(at):
        pltpu.make_async_copy(rn_ref.at[at], rbuf.at[me], lsem.at[0]).start()
        pltpu.make_async_copy(dy_ref.at[at], dbuf.at[me], lsem.at[1]).start()
        for step in range(1, ranks):
            rank = lax.rem(me + step, ranks)
            pltpu.make_async_copy(gath_ref.at[0, rank, at], rbuf.at[rank], lsem.at[0]).start()
            pltpu.make_async_copy(gath_ref.at[1, rank, at], dbuf.at[rank], lsem.at[1]).start()

    def keep_own(at):
        return (pltpu.make_async_copy(rbuf.at[me], gath_ref.at[0, me, at], gsem.at[0]),
                pltpu.make_async_copy(dbuf.at[me], gath_ref.at[1, me, at], gsem.at[1]))

    def table_copy(target):
        return pltpu.make_async_remote_copy(src_ref=tab_ref, dst_ref=tabs.at[me], send_sem=tsend.at[target],
                                            recv_sem=trecv.at[me], device_id={'sp': target}, device_id_type=MESH)

    def weight_copies():
        return (pltpu.make_async_copy(wqkv_ref.at[:, lane(core, q_cols)], wq_s.at[:, pl.ds(0, q_cols)], wsem.at[0]),
                pltpu.make_async_copy(wqkv_ref.at[:, pl.ds(pl.multiple_of(q_dim + core * k_cols, 128), k_cols)],
                                      wq_s.at[:, pl.ds(q_cols, k_cols)], wsem.at[1]),
                pltpu.make_async_copy(wqkv_ref.at[:, pl.ds(pl.multiple_of(q_dim + kv_dim + core * k_cols, 128), k_cols)],
                                      wq_s.at[:, pl.ds(q_cols + k_cols, k_cols)], wsem.at[2]),
                pltpu.make_async_copy(wout_ref.at[pl.ds(pl.multiple_of(core * q_cols, 128), q_cols)], wo_s, wsem.at[3]))

    @pl.when(b == 0)
    def _():
        for copy in weight_copies():
            copy.start()
        own_table = pltpu.make_async_copy(tab_ref, tabs.at[me], wsem.at[4])
        own_table.start()
        barrier = pltpu.get_barrier_semaphore()
        for step in range(1, ranks):
            pl.semaphore_signal(barrier, inc=1, device_id={'sp': lax.rem(me + step, ranks)}, device_id_type=MESH)
        pl.semaphore_wait(barrier, ranks - 1)
        direct(0)
        for step in range(1, ranks):
            table_copy(lax.rem(me + step, ranks)).start()
        relay_near(0)
        direct(1)
        direct(2)
        share_near(0)
        own_table.wait()
        for step in range(1, ranks):
            rank = lax.rem(me + step, ranks)
            pltpu.make_async_remote_copy(src_ref=tab_ref, dst_ref=tabs.at[rank], send_sem=tsend.at[rank],
                                         recv_sem=trecv.at[rank], device_id={'sp': rank}, device_id_type=MESH).wait()
        tab = tabs[...].reshape(seq, hd)
        turned = pltpu.roll(tab, hd // 2, 1)
        low = lax.broadcasted_iota(jnp.int32, (seq, hd), 1) < hd // 2
        cos_s[...] = jnp.where(low, tab, turned)
        sin_s[...] = jnp.where(low, -turned, tab)
        relay_far(0)
        wait_shared(0)
        load(0)
        for copy in weight_copies():
            copy.wait()

    @pl.when(b + 1 < nb)
    def _():
        relay_near(b + 1)

    @pl.when(b + 3 < nb)
    def _():
        direct(b + 3)

    @pl.when(b + 1 < nb)
    def _():
        share_near(b + 1)

    pltpu.make_async_copy(rbuf, rbuf, lsem.at[0]).wait()
    pltpu.make_async_copy(dbuf, dbuf, lsem.at[1]).wait()
    for copy in keep_own(b):
        copy.start()
    qkv_s[...] = dot_nn(rbuf[...].reshape(seq, dim), wq_s[...]).astype(BF16)
    do_s[...] = dot_nt(dbuf[...].reshape(seq, dim), wo_s[...]).astype(BF16)

    nblk = seq // QB
    rpb = QB // tl
    rows_blk = group * QB
    score_scale = hd ** -0.5
    exp_scale = score_scale * math.log2(math.e)
    row_ids = lax.broadcasted_iota(jnp.int32, (QB, QB), 0)
    col_ids = lax.broadcasted_iota(jnp.int32, (QB, QB), 1)
    causal = row_ids >= col_ids
    lanes = ks.shape[0]

    def rope(vals, rows):
        wide = vals.astype(F32)
        return (wide * cos_s[rows] + pltpu.roll(wide, hd // 2, 1) * sin_s[rows]).astype(BF16)

    def rope_back(vals, rows):
        wide = vals.astype(BF16).astype(F32)
        return (wide * cos_s[rows] - pltpu.roll(wide, hd // 2, 1) * sin_s[rows]).astype(BF16)

    def one_pair(pair, carry):
        def q_at(s, g):
            return lane((pair * lanes + s) * group + g, hd)

        def k_at(s):
            return pl.ds(pl.multiple_of(q_cols + (pair * lanes + s) * hd, hd), hd)

        def v_at(s):
            return pl.ds(pl.multiple_of(q_cols + k_cols + (pair * lanes + s) * hd, hd), hd)

        def prepare(s):
            ks[s] = rope(qkv_s[:, k_at(s)], pl.ds(0, seq))
            for g in range(group):
                for blk in range(nblk):
                    rows = pl.ds(blk * QB, QB)
                    dst = pl.ds(blk * rows_blk + g * QB, QB)
                    qs[s, dst] = rope(qkv_s[rows, q_at(s, g)], rows)
                    dos[s, dst] = do_s[rows, q_at(s, g)]

        def softmax(s, blk):
            span = (blk + 1) * QB
            rows = pl.ds(blk * rows_blk, rows_blk)
            sc[s, :, :span] = dot_nt(qs[s, rows], ks[s, :span])
            gps[s, :, :span] = dot_nt(dos[s, rows], qkv_s[:span, v_at(s)]).astype(BF16)
            for g in range(group):
                part = slice(g * QB, (g + 1) * QB)
                dst = pl.ds(blk * rows_blk + g * QB, QB)
                scores = sc[s, part, :span]
                diag = jnp.where(causal, scores[:, span - QB:], -jnp.inf)
                scores = diag if blk == 0 else jnp.concatenate([scores[:, :span - QB], diag], axis=1)
                top = jnp.max(scores, axis=1, keepdims=True)
                ex = jnp.exp2((scores - top) * exp_scale)
                probs = ex * (1.0 / jnp.sum(ex, axis=1, keepdims=True))
                ps[s, dst, :span] = probs.astype(BF16)
                gp = gps[s, part, :span].astype(F32)
                rdot = jnp.sum(gp * probs, axis=1, keepdims=True)
                dss[s, dst, :span] = (probs * (gp - rdot) * score_scale).astype(BF16)

        def by_query(s, blk):
            span = (blk + 1) * QB
            rows = pl.ds(blk * rows_blk, rows_blk)
            outs = dot_nn(ps[s, rows, :span], qkv_s[:span, v_at(s)]).astype(BF16)
            gq = dot_nn(dss[s, rows, :span], ks[s, :span])
            for g in range(group):
                part = slice(g * QB, (g + 1) * QB)
                o_ref[blk * rpb:(blk + 1) * rpb, 0, :, q_at(s, g)] = outs[part].reshape(rpb, tl, hd)
                back = rope_back(gq[part], pl.ds(blk * QB, QB)).reshape(rpb, tl, hd)
                dqkv_ref[blk * rpb:(blk + 1) * rpb, 0, :, q_at(s, g)] = back

        def by_key(s, blk):
            rows = pl.ds(blk * rows_blk, (nblk - blk) * rows_blk)
            cols = slice(blk * QB, (blk + 1) * QB)
            gv = dot_tn(ps[s, rows, cols], dos[s, rows]).astype(BF16).reshape(rpb, tl, hd)
            gk = rope_back(dot_tn(dss[s, rows, cols], qs[s, rows]), pl.ds(blk * QB, QB)).reshape(rpb, tl, hd)
            dqkv_ref[blk * rpb:(blk + 1) * rpb, 0, :, v_at(s)] = gv
            dqkv_ref[blk * rpb:(blk + 1) * rpb, 0, :, k_at(s)] = gk

        for s in range(lanes):
            prepare(s)
        for blk in range(nblk - 1, -1, -1):
            for work in (softmax, by_query, by_key):
                for s in range(lanes):
                    work(s, blk)

        @pl.when((pair == 0) & (b + 1 < nb))
        def _():
            for copy in keep_own(b):
                copy.wait()
            wait_shared(b + 1)
            load(b + 1)
        return carry

    @pl.when(b + 1 < nb)
    def _():
        relay_far(b + 1)

    lax.fori_loop(0, slots // lanes, one_pair, 0)
    osend_ref[0] = o_ref[peer, 0]
    gsend_ref[0] = dqkv_ref[peer, 0]

    @pl.when(b == nb - 1)
    def _():
        for copy in keep_own(b):
            copy.wait()

        def drain(at, carry):
            for kind, rank in ((0, me), (1, me), (4, me), (5, left), (6, right), (7, far)):
                rcopy(both(rank, at), both(rank, at), kind, at, me).wait_send()
            for kind in (2, 3):
                rcopy(gath_ref.at[0, me, at], gath_ref.at[0, me, at], kind, at, me).wait_send()
            return carry
        lax.fori_loop(0, nb, drain, 0)


def attend(normed, grad_out, w_qkv, w_out, table, ranks):
    nb, tl, dim = normed.shape
    hd = table.shape[1]
    seq = ranks * tl
    q_cols, k_cols = w_out.shape[0] // 2, (w_qkv.shape[1] - w_out.shape[0]) // 4
    slots = k_cols // hd
    group = q_cols // k_cols
    cols = q_cols + 2 * k_cols
    lanes = math.gcd(2, slots)
    flops = 2 * nb * seq * dim * (cols + q_cols) + 2 * 6 * nb * slots * group * seq * seq * hd
    return pl.pallas_call(
        functools.partial(attend_kernel, ranks, slots, group, hd, nb),
        grid=(nb,),
        in_specs=[ANY] * 5,
        out_specs=[ANY, pl.BlockSpec((ranks, 1, tl, q_cols), lambda b: (0, b, 0, 0)),
                   pl.BlockSpec((ranks, 1, tl, cols), lambda b: (0, b, 0, 0)),
                   pl.BlockSpec((1, tl, q_cols), lambda b: (b, 0, 0)), pl.BlockSpec((1, tl, cols), lambda b: (b, 0, 0))],
        out_shape=[jax.ShapeDtypeStruct((2, ranks, nb, tl, dim), BF16),
                   jax.ShapeDtypeStruct((ranks, nb, tl, q_cols), BF16),
                   jax.ShapeDtypeStruct((ranks, nb, tl, cols), BF16),
                   jax.ShapeDtypeStruct((nb, tl, q_cols), BF16), jax.ShapeDtypeStruct((nb, tl, cols), BF16)],
        scratch_shapes=[pltpu.VMEM((dim, cols), BF16), pltpu.VMEM((q_cols, dim), BF16),
                        pltpu.VMEM((ranks, tl, dim), BF16), pltpu.VMEM((ranks, tl, dim), BF16),
                        pltpu.VMEM((ranks, tl, hd), F32), pltpu.VMEM((seq, hd), F32), pltpu.VMEM((seq, hd), F32),
                        pltpu.VMEM((seq, cols), BF16), pltpu.VMEM((seq, q_cols), BF16),
                        pltpu.VMEM((lanes, group * seq, hd), BF16), pltpu.VMEM((lanes, group * seq, hd), BF16),
                        pltpu.VMEM((lanes, seq, hd), BF16),
                        pltpu.VMEM((lanes, group * seq, seq), BF16), pltpu.VMEM((lanes, group * seq, seq), BF16),
                        pltpu.VMEM((lanes, group * QB, seq), F32), pltpu.VMEM((lanes, group * QB, seq), BF16),
                        pltpu.SemaphoreType.DMA((8, nb)), pltpu.SemaphoreType.DMA((8, nb)),
                        pltpu.SemaphoreType.DMA((ranks,)), pltpu.SemaphoreType.DMA((ranks,)),
                        pltpu.SemaphoreType.DMA((5,)), pltpu.SemaphoreType.DMA((2,)), pltpu.SemaphoreType.DMA((2,))],
        compiler_params=pltpu.CompilerParams(dimension_semantics=("arbitrary",), vmem_limit_bytes=VMEM_LIMIT,
                                             collective_id=0, has_side_effects=True),
        cost_estimate=pl.CostEstimate(flops=flops, bytes_accessed=2 * nb * seq * (4 * dim + cols + q_cols),
                                      transcendentals=nb * slots * group * seq * seq),
        name="attend",
    )(normed, grad_out, w_qkv, w_out, table)


class Placer:
    def __init__(self, recv, full, buf, sems, steps, pieces):
        self.recv, self.full, self.buf, self.sems, self.steps, self.pieces = recv, full, buf, sems, steps, pieces
        self.rows = recv.shape[0] // steps

    def take(self, step):
        at = pl.ds(pl.multiple_of(step * self.rows, 8), self.rows)
        return pltpu.make_async_copy(self.recv.at[at], self.buf.at[lax.rem(step, 2)], self.sems.at[0, lax.rem(step, 2)])

    def put(self, step):
        out = []
        slot = lax.rem(step, 2)
        for n, (src_col, width, dst) in enumerate(self.pieces):
            out.append(pltpu.make_async_copy(self.buf.at[slot, :, pl.ds(src_col, width)], self.full.at[dst(step * self.rows, self.rows, width)],
                                             self.sems.at[1 + n, slot]))
        return out

    def first(self):
        self.take(0).start()

    def step(self, step):
        self.take(step).wait()
        for copy in self.put(step):
            copy.start()

        @pl.when(step >= 1)
        def _():
            for copy in self.put(step - 1):
                copy.wait()

        @pl.when(step + 1 < self.steps)
        def _():
            self.take(step + 1).start()

    def last(self):
        for copy in self.put(self.steps - 1):
            copy.wait()


def peer_cols(base, stride):
    def where(row, rows, width):
        return (pl.ds(pl.multiple_of(row, 8), rows), pl.ds(pl.multiple_of(base + (1 - my_core()) * stride, 128), width))
    return where


def peer_rows(stride):
    def where(row, rows, width):
        return (pl.ds(pl.multiple_of((1 - my_core()) * stride + row, 8), rows), pl.ds(0, width))
    return where


def weight_grad_kernel(total, left_at, right_at, chunks, pieces, placing, n_in, n_out, *refs):
    left_ref, right_ref = refs[0], refs[1]
    outs = refs[n_in:n_in + n_out]
    lbuf, rbuf, acc, sems = refs[n_in + n_out:n_in + n_out + 4]
    extra = refs[n_in + n_out + 4:]
    placers = [Placer(refs[src], outs[dst], extra[2 * n], extra[2 * n + 1], total, place_pieces)
               for n, (src, dst, place_pieces) in enumerate(placing)]

    def fetch(step, slot):
        return (pltpu.make_async_copy(left_ref.at[left_at(step)], lbuf.at[slot], sems.at[0, slot]),
                pltpu.make_async_copy(right_ref.at[right_at(step)], rbuf.at[slot], sems.at[1, slot]))

    def flat(buf, slot):
        val = buf[slot]
        return val.reshape(-1, val.shape[-1])

    for copy in fetch(0, 0):
        copy.start()
    for placer in placers:
        placer.first()
    acc[...] = jnp.zeros_like(acc)

    def body(step, carry):
        slot = lax.rem(step, 2)
        for copy in fetch(step + 1, 1 - slot):
            copy.start()
        for copy in fetch(step, slot):
            copy.wait()
        for placer in placers:
            placer.step(step)
        acc[...] += dot_tn(flat(lbuf, slot), flat(rbuf, slot))
        return carry

    lax.fori_loop(0, total - 2, body, 0)
    ends = ((total - 2) % 2, (total - 1) % 2)
    for copy in fetch(total - 1, ends[1]):
        copy.start()
    for n, slot in enumerate(ends):
        for copy in fetch(total - 2 + n, slot):
            copy.wait()
        for placer in placers:
            placer.step(jnp.int32(total - 2 + n))
    copies = []
    part = acc.shape[0] // chunks
    for n in range(chunks):
        rows = pl.ds(n * part, part)
        for slot in ends:
            val = lbuf[slot, :, :, n * part:(n + 1) * part]
            acc[rows] += dot_tn(val.reshape(-1, part), flat(rbuf, slot))
        for m, (out, src_col, width, dst) in enumerate(pieces):
            copy = pltpu.make_async_copy(acc.at[rows, pl.ds(src_col, width)], outs[out].at[dst(n * part, part, width)],
                                         sems.at[2 + m, n])
            copy.start()
            copies.append(copy)
    for copy in copies:
        copy.wait()
    for placer in placers:
        placer.last()


def weight_grad(left, right, left_sel, right_sel, acc_shape, chunks, pieces, full_struct, carried, places, order, name):
    ranks, nb, tl = right.shape[-4], right.shape[-3], right.shape[-2]

    def at(sel, ref):
        if sel[0] == "plane":
            return (lambda step: (sel[1], slice(None), step)), ref.shape[-1]
        return (lambda step: (slice(None), step, slice(None), pl.ds(sel[1], sel[2]))), sel[2]
    left_at, left_width = at(left_sel, left)
    right_at, right_width = at(right_sel, right)
    operands, aliases = [left, right], {}
    out_shape = [full_struct, jax.ShapeDtypeStruct(acc_shape, F32)]
    scratch = [pltpu.VMEM((2, ranks, tl, left_width), BF16), pltpu.VMEM((2, ranks, tl, right_width), BF16),
               pltpu.VMEM(acc_shape, F32), pltpu.SemaphoreType.DMA((2 + len(pieces), max(2, chunks)))]
    placing = []
    for recv, full, place_pieces in places:
        src, dst = len(operands), 0
        operands.append(recv)
        if full is not None:
            dst = len(out_shape)
            aliases[len(operands)] = dst
            operands.append(full)
            out_shape.append(jax.ShapeDtypeStruct(full.shape, F32))
        placing.append((src, dst, place_pieces))
        scratch += [pltpu.VMEM((2, recv.shape[0] // nb, recv.shape[1]), F32),
                    pltpu.SemaphoreType.DMA((1 + len(place_pieces), 2))]
    if carried is not None:
        aliases[len(operands)] = 0
        operands.append(carried)
    operands += order
    rows = ranks * nb * tl
    return pl.pallas_call(
        functools.partial(weight_grad_kernel, nb, left_at, right_at, chunks, pieces, placing, len(operands), len(out_shape)),
        in_specs=[ANY] * len(operands),
        out_specs=[ANY] * len(out_shape),
        out_shape=out_shape,
        scratch_shapes=scratch,
        input_output_aliases=aliases,
        compiler_params=pltpu.CompilerParams(vmem_limit_bytes=VMEM_LIMIT),
        cost_estimate=pl.CostEstimate(flops=2 * rows * acc_shape[0] * acc_shape[1],
                                      bytes_accessed=2 * rows * (left_width + right_width) + 8 * acc_shape[0] * acc_shape[1],
                                      transcendentals=0),
        name=name,
    )(*operands)


def canonical_copies(mine_ref, pair_ref, full, sems, parts):
    core, me = my_core(), lax.axis_index('sp')
    out, src, base = [], 0, 0
    for n, width in enumerate(parts):
        for side, ref in enumerate((mine_ref.at[me], pair_ref)):
            owner = core if side == 0 else 1 - core
            dst = pl.ds(pl.multiple_of(base + owner * width, 128), width)
            out.append(pltpu.make_async_copy(ref.at[:, :, pl.ds(src, width)], full.at[:, :, dst], sems.at[n, side]))
        src += width
        base += 2 * width
    return out


def hidden_grad_kernel(parts, w_ref, x_ref, inv_ref, gain_ref, gm_ref, gp_ref, dy_ref, order_ref,
                       dx_ref, dg_ref, gfull, dn_s, xs, dys, mean_s, csem, dsem):
    del order_ref
    step = pl.program_id(0)
    steps = pl.num_programs(0)
    nb, tl, dim = dys.shape
    rows = nb * tl
    width = w_ref.shape[0]

    @pl.when(step == 0)
    def _():
        for copy in canonical_copies(gm_ref, gp_ref, gfull, csem, parts):
            copy.start()
        pltpu.make_async_copy(x_ref, xs, dsem.at[0]).start()
        pltpu.make_async_copy(dy_ref, dys, dsem.at[1]).start()
        mean_s[...] = jnp.zeros_like(mean_s)
        for copy in canonical_copies(gm_ref, gp_ref, gfull, csem, parts):
            copy.wait()

    at = lane(step, width)
    dn_s[:, at] = dot_nt(gfull[...].reshape(rows, gfull.shape[-1]), w_ref[...]).astype(BF16)

    @pl.when(step == 0)
    def _():
        pltpu.make_async_copy(x_ref, xs, dsem.at[0]).wait()

    grad = dn_s[:, at].astype(F32)
    unit = xs[:, :, at].reshape(rows, width).astype(F32) * inv_ref[...]
    prod = grad * unit
    mean_s[...] += jnp.sum(prod * gain_ref[:, at], axis=1, keepdims=True)
    dg_ref[:, at] = jnp.sum(prod, axis=0, keepdims=True)

    @pl.when(step == steps - 1)
    def _():
        pltpu.make_async_copy(dy_ref, dys, dsem.at[1]).wait()

        def finish(i, carry):
            for sub in range(tl // 16):
                here = pl.ds(sub * 16, 16)
                span = pl.ds(pl.multiple_of(i * tl + sub * 16, 16), 16)
                inv = inv_ref[span]
                unit_rows = xs[i, here].astype(F32) * inv
                inner = inv * (dn_s[span].astype(F32) * gain_ref[...] - unit_rows * (mean_s[span] * (1.0 / dim)))
                dys[i, here] = (dys[i, here].astype(F32) + inner).astype(BF16)
            pltpu.make_async_copy(dys.at[i], dx_ref.at[i], dsem.at[2]).start()
            return carry
        lax.fori_loop(0, nb, finish, 0)
        pltpu.make_async_copy(dys, dx_ref, dsem.at[2]).wait()


def hidden_grad(hidden, grad_out, inv_rms, norm_weight, w_qkv, g_all, g_pair, parts, order):
    nb, tl, dim = hidden.shape
    cols = w_qkv.shape[1]
    width = 512
    const = lambda *shape: pl.BlockSpec(shape, lambda n: (0,) * len(shape), pipeline_mode=pl.Buffered(1))
    return pl.pallas_call(
        functools.partial(hidden_grad_kernel, parts),
        grid=(dim // width,),
        in_specs=[pl.BlockSpec((width, cols), lambda n: (n, 0)), ANY, const(nb * tl, 1), const(1, dim),
                  ANY, ANY, ANY, ANY],
        out_specs=[ANY, const(1, dim)],
        out_shape=[jax.ShapeDtypeStruct((nb, tl, dim), BF16), jax.ShapeDtypeStruct((1, dim), F32)],
        scratch_shapes=[pltpu.VMEM((nb, tl, cols), BF16), pltpu.VMEM((nb * tl, dim), BF16), pltpu.VMEM((nb, tl, dim), BF16),
                        pltpu.VMEM((nb, tl, dim), BF16), pltpu.VMEM((nb * tl, 1), F32),
                        pltpu.SemaphoreType.DMA((len(parts), 2)), pltpu.SemaphoreType.DMA((3,))],
        compiler_params=pltpu.CompilerParams(dimension_semantics=("arbitrary",), vmem_limit_bytes=VMEM_LIMIT),
        cost_estimate=pl.CostEstimate(flops=2 * nb * tl * dim * cols, bytes_accessed=2 * dim * cols, transcendentals=0),
        name="hidden_grad",
    )(w_qkv, hidden, inv_rms, norm_weight, g_all, g_pair, grad_out, order)


def project_out_kernel(parts, w_ref, x_ref, om_ref, op_ref, order_ref, y_ref, ofull, csem):
    del order_ref
    nb, tl, q_dim = ofull.shape

    @pl.when(pl.program_id(0) == 0)
    def _():
        for copy in canonical_copies(om_ref, op_ref, ofull, csem, parts):
            copy.start()
        for copy in canonical_copies(om_ref, op_ref, ofull, csem, parts):
            copy.wait()

    mixed = dot_nn(ofull[...].reshape(nb * tl, q_dim), w_ref[...])
    y_ref[...] = (x_ref[...].astype(F32) + mixed.reshape(y_ref.shape)).astype(BF16)


def project_out(hidden, w_out, o_all, o_pair, parts, order):
    nb, tl, dim = hidden.shape
    q_dim = w_out.shape[0]
    width = 512
    tile = pl.BlockSpec((nb, tl, width), lambda n: (0, 0, n))
    return pl.pallas_call(
        functools.partial(project_out_kernel, parts),
        grid=(dim // width,),
        in_specs=[pl.BlockSpec((q_dim, width), lambda n: (0, n)), tile, ANY, ANY, ANY],
        out_specs=tile,
        out_shape=jax.ShapeDtypeStruct((nb, tl, dim), BF16),
        scratch_shapes=[pltpu.VMEM((nb, tl, q_dim), BF16), pltpu.SemaphoreType.DMA((len(parts), 2))],
        compiler_params=pltpu.CompilerParams(dimension_semantics=("arbitrary",), vmem_limit_bytes=VMEM_LIMIT),
        cost_estimate=pl.CostEstimate(flops=2 * nb * tl * dim * q_dim, bytes_accessed=2 * dim * q_dim, transcendentals=0),
        name="project_out",
    )(w_out, hidden, o_all, o_pair, order)


def place_kernel(steps, place_pieces, recv_ref, full_in, full_ref, bounce, sems):
    del full_in
    placer = Placer(recv_ref, full_ref, bounce, sems, steps, place_pieces)
    placer.first()

    def body(step, carry):
        placer.step(step)
        return carry
    lax.fori_loop(0, steps, body, 0)
    placer.last()


def place(recv, full, place_pieces, steps):
    return pl.pallas_call(
        functools.partial(place_kernel, steps, place_pieces),
        in_specs=[ANY, ANY],
        out_specs=ANY,
        out_shape=jax.ShapeDtypeStruct(full.shape, F32),
        scratch_shapes=[pltpu.VMEM((2, recv.shape[0] // steps, recv.shape[1]), F32),
                        pltpu.SemaphoreType.DMA((1 + len(place_pieces), 2))],
        input_output_aliases={1: 0},
        compiler_params=pltpu.CompilerParams(vmem_limit_bytes=VMEM_LIMIT),
        cost_estimate=pl.CostEstimate(flops=recv.size, bytes_accessed=8 * recv.size, transcendentals=0),
        name="place",
    )(recv, full)


def group_sum_kernel(ranks, part_ref, sum_ref, parts, ssem, rsem):
    me = lax.axis_index('sp')
    barrier = pltpu.get_barrier_semaphore()
    for step in range(1, ranks):
        pl.semaphore_signal(barrier, inc=1, device_id={'sp': lax.rem(me + step, ranks)}, device_id_type=MESH)
    pl.semaphore_wait(barrier, ranks - 1)

    def copy(slot, target):
        return pltpu.make_async_remote_copy(src_ref=part_ref, dst_ref=parts.at[slot], send_sem=ssem.at[target],
                                            recv_sem=rsem.at[slot], device_id={'sp': target}, device_id_type=MESH)
    own = pltpu.make_async_copy(part_ref, parts.at[me], ssem.at[me])
    own.start()
    for step in range(1, ranks):
        copy(me, lax.rem(me + step, ranks)).start()
    own.wait()
    for step in range(1, ranks):
        rank = lax.rem(me + step, ranks)
        copy(rank, rank).wait()
    total = parts[0]
    for rank in range(1, ranks):
        total = total + parts[rank]
    sum_ref[...] = total


def group_sum(part, ranks):
    return pl.pallas_call(
        functools.partial(group_sum_kernel, ranks),
        in_specs=[ANY],
        out_specs=pl.BlockSpec(memory_space=pltpu.VMEM),
        out_shape=jax.ShapeDtypeStruct(part.shape, F32),
        scratch_shapes=[pltpu.VMEM((ranks,) + part.shape, F32), pltpu.SemaphoreType.DMA((ranks,)),
                        pltpu.SemaphoreType.DMA((ranks,))],
        compiler_params=pltpu.CompilerParams(collective_id=1, has_side_effects=True),
        cost_estimate=pl.CostEstimate(flops=ranks * part.size, bytes_accessed=8 * ranks * part.size, transcendentals=0),
        name="group_sum",
    )(part)


def block_body(ranks, hidden, positions, long_factor, norm_weight, w_qkv, w_out, grad_out):
    nb, tl, dim = hidden.shape
    hd = 2 * long_factor.shape[0]
    q_dim = w_out.shape[0]
    kv_dim = (w_qkv.shape[1] - q_dim) // 2
    pair = [(i, i ^ 1) for i in range(ranks)]
    qh, kh = q_dim // 2, kv_dim // 2

    hidden_wide = hidden.astype(F32)
    inv_rms = lax.rsqrt(jnp.mean(hidden_wide * hidden_wide, axis=-1, keepdims=True) + NORM_EPS)
    normed = (hidden_wide * inv_rms * norm_weight).astype(BF16)
    gathered, o_all, g_all, o_send, g_send = attend(normed, grad_out, w_qkv, w_out,
                                                    half_tables(positions, long_factor), ranks)
    o_pair = lax.ppermute(o_send, 'sp', pair)
    g_pair = lax.ppermute(g_send, 'sp', pair)

    def own_cols(base, stride):
        def where(row, rows, width):
            return (pl.ds(row, rows), pl.ds(pl.multiple_of(base + my_core() * stride, 128), width))
        return where

    def own_rows(stride):
        def where(row, rows, width):
            return (pl.ds(pl.multiple_of(my_core() * stride + row, 8), rows), pl.ds(0, width))
        return where

    def same(row, rows, width):
        return (pl.ds(row, rows), pl.ds(0, width))

    dwq_struct = jax.ShapeDtypeStruct(w_qkv.shape, F32)
    dwo_struct = jax.ShapeDtypeStruct(w_out.shape, F32)
    dwq, send_q = weight_grad(gathered, g_all, ("plane", 0), ("cols", 0, qh), (dim, qh), 4,
                              [(0, 0, qh, own_cols(0, qh)), (1, 0, qh, same)], dwq_struct, None, [], [], "wgrad_q")
    recv_q = lax.ppermute(send_q, 'sp', pair)
    dwo, send_o = weight_grad(o_all, gathered, ("cols", 0, qh), ("plane", 1), (qh, dim), 4,
                              [(0, 0, dim, own_rows(qh)), (1, 0, dim, same)], dwo_struct, None, [], [dwq, o_pair, g_pair],
                              "wgrad_out")
    recv_o = lax.ppermute(send_o, 'sp', pair)
    grad_hidden, grad_norm = hidden_grad(hidden, grad_out, inv_rms.reshape(nb * tl, 1), norm_weight[None], w_qkv, g_all,
                                         g_pair, [qh, kh, kh], dwo)
    dwq, send_kv, dwo = weight_grad(gathered, g_all, ("plane", 0), ("cols", qh, 2 * kh), (dim, 2 * kh), 4,
                                    [(0, 0, kh, own_cols(q_dim, kh)), (0, kh, kh, own_cols(q_dim + kv_dim, kh)),
                                     (1, 0, 2 * kh, same)], dwq_struct, dwq,
                                    [(recv_o, dwo, [(0, dim, peer_rows(qh))]), (recv_q, None, [(0, qh, peer_cols(0, qh))])],
                                    [grad_norm], "wgrad_kv")
    recv_kv = lax.ppermute(send_kv, 'sp', pair)
    grad_norm = group_sum(grad_norm.reshape(-1, 128), ranks).reshape(-1)
    out_hidden = project_out(hidden, w_out, o_all, o_pair, [qh], send_kv)
    dwq = place(recv_kv, dwq, [(0, kh, peer_cols(q_dim, kh)), (kh, kh, peer_cols(q_dim + kv_dim, kh))], 8)
    return out_hidden, grad_hidden, grad_norm, dwq, dwo


def solution(mesh):
    token_spec = P('dp', 'sp', None)
    return jax.shard_map(functools.partial(block_body, mesh.shape['sp']), mesh=mesh,
                         in_specs=(token_spec, P(('dp', 'sp')), P(), P(), P(), P(), token_spec),
                         out_specs=(token_spec, token_spec, P('dp'), P('dp', None), P('dp', None)),
                         check_vma=False)
```

```python
import functools
import math
import jax
import jax.numpy as jnp
from jax import lax
from jax.experimental import pallas as pl
from jax.experimental.pallas import tpu as pltpu
from jax.sharding import PartitionSpec as P

NORM_EPS = 1e-5
ROPE_BASE = 10000.0
ROPE_SCALE = math.sqrt(1.0 + math.log(32.0) / math.log(4096.0))
F32 = jnp.float32
BF16 = jnp.bfloat16
MESH = pl.DeviceIdType.MESH
VMEM_LIMIT = 67000000
QB = 128
ANY = pl.BlockSpec(memory_space=pl.ANY)


def dot_nn(a, b):
    return lax.dot_general(a, b, (((1,), (0,)), ((), ())), preferred_element_type=F32)


def dot_nt(a, b):
    return lax.dot_general(a, b, (((1,), (1,)), ((), ())), preferred_element_type=F32)


def dot_tn(a, b):
    return lax.dot_general(a, b, (((0,), (0,)), ((), ())), preferred_element_type=F32)


def lane(index, width):
    return pl.ds(pl.multiple_of(index * width, 128), width)


def my_core():
    return lax.rem(lax.axis_index('sp'), 2)


def half_tables(positions, long_factor):
    half = long_factor.shape[0]
    exponents = jnp.arange(0, 2 * half, 2).astype(F32) / (2 * half)
    inv_freq = 1.0 / (long_factor * ROPE_BASE ** exponents)
    angles = positions.astype(F32)[:, None] * inv_freq
    return jnp.concatenate([jnp.cos(angles) * ROPE_SCALE, jnp.sin(angles) * ROPE_SCALE], axis=-1)


def attend_kernel(ranks, slots, group, hd, nb, x_ref, gain_ref, dy_ref, wqkv_ref, wout_ref, tab_ref, gath_ref, rn_ref, inv_ref, o_ref, dqkv_ref, osend_ref, gsend_ref,
                  wq_s, wo_s, rbuf, dbuf, tabs, cos_s, sin_s, qkv_s, do_s, qs, dos, ks, ps, dss, sc, gps,
                  ssem, rsem, tsend, trecv, wsem, lsem, gsem, xsem, nsem):
    b = pl.program_id(0)
    tl, dim = dy_ref.shape[1], dy_ref.shape[2]
    seq = ranks * tl
    q_cols, k_cols = slots * group * hd, slots * hd
    q_dim, kv_dim = 2 * q_cols, 2 * k_cols
    me = lax.axis_index('sp')
    core = lax.rem(me, 2)
    peer = me + 1 - 2 * core
    left, right = lax.rem(me + ranks - 2, ranks), lax.rem(me + 2, ranks)
    far = lax.rem(me + 4, ranks)
    cross = 1 - 2 * core

    def rcopy(src, dst, kind, at, target):
        return pltpu.make_async_remote_copy(src_ref=src, dst_ref=dst, send_sem=ssem.at[kind, at],
                                            recv_sem=rsem.at[kind, at], device_id={'sp': target}, device_id_type=MESH)

    def both(rank, at):
        return gath_ref.at[:, rank, at]

    def direct_part(at, which):
        source = dy_ref if which else rn_ref
        for kind, target in ((0, right), (1, left), (4, peer)):
            rcopy(source.at[at], gath_ref.at[which, me, at], kind, at, target).start()

    def direct(at):
        direct_part(at, 0)
        direct_part(at, 1)

    def x_load(at):
        slot = lax.rem(at, ranks)
        return pltpu.make_async_copy(x_ref.at[at], dbuf.at[slot], xsem.at[slot])

    def norm_store(at):
        slot = lax.rem(at, ranks)
        return pltpu.make_async_copy(rbuf.at[slot], rn_ref.at[at], nsem.at[slot])

    def norm(at):
        slot = lax.rem(at, ranks)
        x_load(at).wait()
        wide = dbuf[slot].astype(F32)
        inv = lax.rsqrt(jnp.mean(wide * wide, axis=1, keepdims=True) + NORM_EPS)
        inv_ref[pl.ds(pl.multiple_of(at * tl, tl), tl)] = inv
        rbuf[slot] = (wide * inv * gain_ref[...]).astype(BF16)

    def relay_near(at):
        rcopy(both(left, at), both(left, at), 0, at, me).wait_recv()
        rcopy(both(right, at), both(right, at), 1, at, me).wait_recv()
        rcopy(gath_ref.at[0, left, at], gath_ref.at[0, left, at], 2, at, right).start()
        rcopy(gath_ref.at[1, right, at], gath_ref.at[1, right, at], 3, at, left).start()

    def share_near(at):
        rcopy(both(left, at), both(left, at), 5, at, peer).start()
        rcopy(both(right, at), both(right, at), 6, at, peer).start()

    def relay_far(at):
        rcopy(gath_ref.at[0, far, at], gath_ref.at[0, far, at], 2, at, me).wait_recv()
        rcopy(gath_ref.at[1, far, at], gath_ref.at[1, far, at], 3, at, me).wait_recv()
        rcopy(both(far, at), both(far, at), 7, at, peer).start()

    def wait_shared(at):
        for kind, rank in ((4, peer), (5, left + cross), (6, right + cross), (7, far + cross)):
            rcopy(both(rank, at), both(rank, at), kind, at, me).wait_recv()

    def load(at):
        pltpu.make_async_copy(rn_ref.at[at], rbuf.at[me], lsem.at[0]).start()
        pltpu.make_async_copy(dy_ref.at[at], dbuf.at[me], lsem.at[1]).start()
        for step in range(1, ranks):
            rank = lax.rem(me + step, ranks)
            pltpu.make_async_copy(gath_ref.at[0, rank, at], rbuf.at[rank], lsem.at[0]).start()
            pltpu.make_async_copy(gath_ref.at[1, rank, at], dbuf.at[rank], lsem.at[1]).start()

    def keep_own(at):
        return (pltpu.make_async_copy(rbuf.at[me], gath_ref.at[0, me, at], gsem.at[0]),
                pltpu.make_async_copy(dbuf.at[me], gath_ref.at[1, me, at], gsem.at[1]))

    def table_copy(target):
        return pltpu.make_async_remote_copy(src_ref=tab_ref, dst_ref=tabs.at[me], send_sem=tsend.at[target],
                                            recv_sem=trecv.at[me], device_id={'sp': target}, device_id_type=MESH)

    def weight_copies():
        return (pltpu.make_async_copy(wqkv_ref.at[:, lane(core, q_cols)], wq_s.at[:, pl.ds(0, q_cols)], wsem.at[0]),
                pltpu.make_async_copy(wqkv_ref.at[:, pl.ds(pl.multiple_of(q_dim + core * k_cols, 128), k_cols)],
                                      wq_s.at[:, pl.ds(q_cols, k_cols)], wsem.at[1]),
                pltpu.make_async_copy(wqkv_ref.at[:, pl.ds(pl.multiple_of(q_dim + kv_dim + core * k_cols, 128), k_cols)],
                                      wq_s.at[:, pl.ds(q_cols + k_cols, k_cols)], wsem.at[2]),
                pltpu.make_async_copy(wout_ref.at[pl.ds(pl.multiple_of(core * q_cols, 128), q_cols)], wo_s, wsem.at[3]))

    @pl.when(b == 0)
    def _():
        for copy in weight_copies():
            copy.start()
        own_table = pltpu.make_async_copy(tab_ref, tabs.at[me], wsem.at[4])
        own_table.start()
        first = min(nb, ranks)
        for at in range(first):
            x_load(at).start()
        barrier = pltpu.get_barrier_semaphore()
        for step in range(1, ranks):
            pl.semaphore_signal(barrier, inc=1, device_id={'sp': lax.rem(me + step, ranks)}, device_id_type=MESH)
        pl.semaphore_wait(barrier, ranks - 1)
        direct_part(0, 1)
        norm(0)
        norm(1)
        norm_store(0).start()
        norm_store(1).start()
        norm_store(0).wait()
        direct_part(0, 0)
        for step in range(1, ranks):
            table_copy(lax.rem(me + step, ranks)).start()

        def norm_more(at, carry):
            norm(at)

            @pl.when(at >= 3)
            def _():
                norm_store(at - 1).start()
            return carry
        lax.fori_loop(2, first, norm_more, 0)
        norm_store(first - 1).start()
        if nb > ranks:
            norm_store(1).wait()
            for at in range(2, ranks):
                norm_store(at).wait()
            for at in range(ranks, nb):
                x_load(at).start()

            def norm_rest(at, carry):
                norm(at)

                @pl.when(at >= ranks + 1)
                def _():
                    norm_store(at - 1).start()
                return carry
            lax.fori_loop(ranks, nb, norm_rest, 0)
            norm_store(nb - 1).start()
            for at in range(ranks, nb):
                norm_store(at).wait()
        else:
            for at in range(1, nb):
                norm_store(at).wait()
        relay_near(0)
        direct(1)
        direct(2)
        share_near(0)
        own_table.wait()
        for step in range(1, ranks):
            rank = lax.rem(me + step, ranks)
            pltpu.make_async_remote_copy(src_ref=tab_ref, dst_ref=tabs.at[rank], send_sem=tsend.at[rank],
                                         recv_sem=trecv.at[rank], device_id={'sp': rank}, device_id_type=MESH).wait()
        tab = tabs[...].reshape(seq, hd)
        turned = pltpu.roll(tab, hd // 2, 1)
        low = lax.broadcasted_iota(jnp.int32, (seq, hd), 1) < hd // 2
        cos_s[...] = jnp.where(low, tab, turned)
        sin_s[...] = jnp.where(low, -turned, tab)
        relay_far(0)
        wait_shared(0)
        load(0)
        for copy in weight_copies():
            copy.wait()

    @pl.when(b + 1 < nb)
    def _():
        relay_near(b + 1)

    @pl.when(b + 3 < nb)
    def _():
        direct(b + 3)

    @pl.when(b + 1 < nb)
    def _():
        share_near(b + 1)

    pltpu.make_async_copy(rbuf, rbuf, lsem.at[0]).wait()
    pltpu.make_async_copy(dbuf, dbuf, lsem.at[1]).wait()
    for copy in keep_own(b):
        copy.start()
    qkv_s[...] = dot_nn(rbuf[...].reshape(seq, dim), wq_s[...]).astype(BF16)
    do_s[...] = dot_nt(dbuf[...].reshape(seq, dim), wo_s[...]).astype(BF16)

    nblk = seq // QB
    rpb = QB // tl
    rows_blk = group * QB
    score_scale = hd ** -0.5
    exp_scale = score_scale * math.log2(math.e)
    row_ids = lax.broadcasted_iota(jnp.int32, (QB, QB), 0)
    col_ids = lax.broadcasted_iota(jnp.int32, (QB, QB), 1)
    causal = row_ids >= col_ids
    lanes = ks.shape[0]

    def rope(vals, rows):
        wide = vals.astype(F32)
        return (wide * cos_s[rows] + pltpu.roll(wide, hd // 2, 1) * sin_s[rows]).astype(BF16)

    def rope_back(vals, rows):
        wide = vals.astype(BF16).astype(F32)
        return (wide * cos_s[rows] - pltpu.roll(wide, hd // 2, 1) * sin_s[rows]).astype(BF16)

    def one_pair(pair, carry):
        def q_at(s, g):
            return lane((pair * lanes + s) * group + g, hd)

        def k_at(s):
            return pl.ds(pl.multiple_of(q_cols + (pair * lanes + s) * hd, hd), hd)

        def v_at(s):
            return pl.ds(pl.multiple_of(q_cols + k_cols + (pair * lanes + s) * hd, hd), hd)

        def prepare(s):
            ks[s] = rope(qkv_s[:, k_at(s)], pl.ds(0, seq))
            for g in range(group):
                for blk in range(nblk):
                    rows = pl.ds(blk * QB, QB)
                    dst = pl.ds(blk * rows_blk + g * QB, QB)
                    qs[s, dst] = rope(qkv_s[rows, q_at(s, g)], rows)
                    dos[s, dst] = do_s[rows, q_at(s, g)]

        def softmax(s, blk):
            span = (blk + 1) * QB
            rows = pl.ds(blk * rows_blk, rows_blk)
            sc[s, :, :span] = dot_nt(qs[s, rows], ks[s, :span])
            gps[s, :, :span] = dot_nt(dos[s, rows], qkv_s[:span, v_at(s)]).astype(BF16)
            for g in range(group):
                part = slice(g * QB, (g + 1) * QB)
                dst = pl.ds(blk * rows_blk + g * QB, QB)
                scores = sc[s, part, :span]
                diag = jnp.where(causal, scores[:, span - QB:], -jnp.inf)
                scores = diag if blk == 0 else jnp.concatenate([scores[:, :span - QB], diag], axis=1)
                top = jnp.max(scores, axis=1, keepdims=True)
                ex = jnp.exp2((scores - top) * exp_scale)
                probs = ex * (1.0 / jnp.sum(ex, axis=1, keepdims=True))
                ps[s, dst, :span] = probs.astype(BF16)
                gp = gps[s, part, :span].astype(F32)
                rdot = jnp.sum(gp * probs, axis=1, keepdims=True)
                dss[s, dst, :span] = (probs * (gp - rdot) * score_scale).astype(BF16)

        def by_query(s, blk):
            span = (blk + 1) * QB
            rows = pl.ds(blk * rows_blk, rows_blk)
            outs = dot_nn(ps[s, rows, :span], qkv_s[:span, v_at(s)]).astype(BF16)
            gq = dot_nn(dss[s, rows, :span], ks[s, :span])
            for g in range(group):
                part = slice(g * QB, (g + 1) * QB)
                o_ref[blk * rpb:(blk + 1) * rpb, 0, :, q_at(s, g)] = outs[part].reshape(rpb, tl, hd)
                back = rope_back(gq[part], pl.ds(blk * QB, QB)).reshape(rpb, tl, hd)
                dqkv_ref[blk * rpb:(blk + 1) * rpb, 0, :, q_at(s, g)] = back

        def by_key(s, blk):
            rows = pl.ds(blk * rows_blk, (nblk - blk) * rows_blk)
            cols = slice(blk * QB, (blk + 1) * QB)
            gv = dot_tn(ps[s, rows, cols], dos[s, rows]).astype(BF16).reshape(rpb, tl, hd)
            gk = rope_back(dot_tn(dss[s, rows, cols], qs[s, rows]), pl.ds(blk * QB, QB)).reshape(rpb, tl, hd)
            dqkv_ref[blk * rpb:(blk + 1) * rpb, 0, :, v_at(s)] = gv
            dqkv_ref[blk * rpb:(blk + 1) * rpb, 0, :, k_at(s)] = gk

        for s in range(lanes):
            prepare(s)
        for blk in range(nblk - 1, -1, -1):
            for work in (softmax, by_query, by_key):
                for s in range(lanes):
                    work(s, blk)

        @pl.when((pair == 0) & (b + 1 < nb))
        def _():
            for copy in keep_own(b):
                copy.wait()
            wait_shared(b + 1)
            load(b + 1)
        return carry

    @pl.when(b + 1 < nb)
    def _():
        relay_far(b + 1)

    lax.fori_loop(0, slots // lanes, one_pair, 0)
    osend_ref[0] = o_ref[peer, 0]
    gsend_ref[0] = dqkv_ref[peer, 0]

    @pl.when(b == nb - 1)
    def _():
        for copy in keep_own(b):
            copy.wait()

        def drain(at, carry):
            for kind, rank in ((0, me), (1, me), (4, me), (5, left), (6, right), (7, far)):
                rcopy(both(rank, at), both(rank, at), kind, at, me).wait_send()
            for kind in (2, 3):
                rcopy(gath_ref.at[0, me, at], gath_ref.at[0, me, at], kind, at, me).wait_send()
            return carry
        lax.fori_loop(0, nb, drain, 0)


def attend(hidden, norm_weight, grad_out, w_qkv, w_out, table, ranks):
    nb, tl, dim = hidden.shape
    hd = table.shape[1]
    seq = ranks * tl
    q_cols, k_cols = w_out.shape[0] // 2, (w_qkv.shape[1] - w_out.shape[0]) // 4
    slots = k_cols // hd
    group = q_cols // k_cols
    cols = q_cols + 2 * k_cols
    lanes = math.gcd(2, slots)
    flops = 2 * nb * seq * dim * (cols + q_cols) + 2 * 6 * nb * slots * group * seq * seq * hd
    return pl.pallas_call(
        functools.partial(attend_kernel, ranks, slots, group, hd, nb),
        grid=(nb,),
        in_specs=[ANY, pl.BlockSpec((1, dim), lambda b: (0, 0), pipeline_mode=pl.Buffered(1))] + [ANY] * 4,
        out_specs=[ANY, ANY, pl.BlockSpec((nb * tl, 1), lambda b: (0, 0)), pl.BlockSpec((ranks, 1, tl, q_cols), lambda b: (0, b, 0, 0)),
                   pl.BlockSpec((ranks, 1, tl, cols), lambda b: (0, b, 0, 0)),
                   pl.BlockSpec((1, tl, q_cols), lambda b: (b, 0, 0)), pl.BlockSpec((1, tl, cols), lambda b: (b, 0, 0))],
        out_shape=[jax.ShapeDtypeStruct((2, ranks, nb, tl, dim), BF16), jax.ShapeDtypeStruct((nb, tl, dim), BF16),
                   jax.ShapeDtypeStruct((nb * tl, 1), F32),
                   jax.ShapeDtypeStruct((ranks, nb, tl, q_cols), BF16),
                   jax.ShapeDtypeStruct((ranks, nb, tl, cols), BF16),
                   jax.ShapeDtypeStruct((nb, tl, q_cols), BF16), jax.ShapeDtypeStruct((nb, tl, cols), BF16)],
        scratch_shapes=[pltpu.VMEM((dim, cols), BF16), pltpu.VMEM((q_cols, dim), BF16),
                        pltpu.VMEM((ranks, tl, dim), BF16), pltpu.VMEM((ranks, tl, dim), BF16),
                        pltpu.VMEM((ranks, tl, hd), F32), pltpu.VMEM((seq, hd), F32), pltpu.VMEM((seq, hd), F32),
                        pltpu.VMEM((seq, cols), BF16), pltpu.VMEM((seq, q_cols), BF16),
                        pltpu.VMEM((lanes, group * seq, hd), BF16), pltpu.VMEM((lanes, group * seq, hd), BF16),
                        pltpu.VMEM((lanes, seq, hd), BF16),
                        pltpu.VMEM((lanes, group * seq, seq), BF16), pltpu.VMEM((lanes, group * seq, seq), BF16),
                        pltpu.VMEM((lanes, group * QB, seq), F32), pltpu.VMEM((lanes, group * QB, seq), BF16),
                        pltpu.SemaphoreType.DMA((8, nb)), pltpu.SemaphoreType.DMA((8, nb)),
                        pltpu.SemaphoreType.DMA((ranks,)), pltpu.SemaphoreType.DMA((ranks,)),
                        pltpu.SemaphoreType.DMA((5,)), pltpu.SemaphoreType.DMA((2,)), pltpu.SemaphoreType.DMA((2,)),
                        pltpu.SemaphoreType.DMA((ranks,)), pltpu.SemaphoreType.DMA((ranks,))],
        compiler_params=pltpu.CompilerParams(dimension_semantics=("arbitrary",), vmem_limit_bytes=VMEM_LIMIT,
                                             collective_id=0, has_side_effects=True),
        cost_estimate=pl.CostEstimate(flops=flops, bytes_accessed=2 * nb * seq * (4 * dim + cols + q_cols),
                                      transcendentals=nb * slots * group * seq * seq),
        name="attend",
    )(hidden, norm_weight, grad_out, w_qkv, w_out, table)


class Placer:
    def __init__(self, recv, full, buf, sems, steps, pieces):
        self.recv, self.full, self.buf, self.sems, self.steps, self.pieces = recv, full, buf, sems, steps, pieces
        self.rows = recv.shape[0] // steps

    def take(self, step):
        at = pl.ds(pl.multiple_of(step * self.rows, 8), self.rows)
        return pltpu.make_async_copy(self.recv.at[at], self.buf.at[lax.rem(step, 2)], self.sems.at[0, lax.rem(step, 2)])

    def put(self, step):
        out = []
        slot = lax.rem(step, 2)
        for n, (src_col, width, dst) in enumerate(self.pieces):
            out.append(pltpu.make_async_copy(self.buf.at[slot, :, pl.ds(src_col, width)], self.full.at[dst(step * self.rows, self.rows, width)],
                                             self.sems.at[1 + n, slot]))
        return out

    def first(self):
        self.take(0).start()

    def step(self, step):
        self.take(step).wait()
        for copy in self.put(step):
            copy.start()

        @pl.when(step >= 1)
        def _():
            for copy in self.put(step - 1):
                copy.wait()

        @pl.when(step + 1 < self.steps)
        def _():
            self.take(step + 1).start()

    def last(self):
        for copy in self.put(self.steps - 1):
            copy.wait()


def peer_cols(base, stride):
    def where(row, rows, width):
        return (pl.ds(pl.multiple_of(row, 8), rows), pl.ds(pl.multiple_of(base + (1 - my_core()) * stride, 128), width))
    return where


def peer_rows(stride):
    def where(row, rows, width):
        return (pl.ds(pl.multiple_of((1 - my_core()) * stride + row, 8), rows), pl.ds(0, width))
    return where


def weight_grad_kernel(total, left_at, right_at, chunks, pieces, placing, n_in, n_out, *refs):
    left_ref, right_ref = refs[0], refs[1]
    outs = refs[n_in:n_in + n_out]
    lbuf, rbuf, acc, sems = refs[n_in + n_out:n_in + n_out + 4]
    extra = refs[n_in + n_out + 4:]
    placers = [Placer(refs[src], outs[dst], extra[2 * n], extra[2 * n + 1], total, place_pieces)
               for n, (src, dst, place_pieces) in enumerate(placing)]

    def fetch(step, slot):
        return (pltpu.make_async_copy(left_ref.at[left_at(step)], lbuf.at[slot], sems.at[0, slot]),
                pltpu.make_async_copy(right_ref.at[right_at(step)], rbuf.at[slot], sems.at[1, slot]))

    def flat(buf, slot):
        val = buf[slot]
        return val.reshape(-1, val.shape[-1])

    for copy in fetch(0, 0):
        copy.start()
    for placer in placers:
        placer.first()
    acc[...] = jnp.zeros_like(acc)

    def body(step, carry):
        slot = lax.rem(step, 2)
        for copy in fetch(step + 1, 1 - slot):
            copy.start()
        for copy in fetch(step, slot):
            copy.wait()
        for placer in placers:
            placer.step(step)
        acc[...] += dot_tn(flat(lbuf, slot), flat(rbuf, slot))
        return carry

    lax.fori_loop(0, total - 2, body, 0)
    ends = ((total - 2) % 2, (total - 1) % 2)
    for copy in fetch(total - 1, ends[1]):
        copy.start()
    for n, slot in enumerate(ends):
        for copy in fetch(total - 2 + n, slot):
            copy.wait()
        for placer in placers:
            placer.step(jnp.int32(total - 2 + n))
    copies = []
    part = acc.shape[0] // chunks
    for n in range(chunks):
        rows = pl.ds(n * part, part)
        for slot in ends:
            val = lbuf[slot, :, :, n * part:(n + 1) * part]
            acc[rows] += dot_tn(val.reshape(-1, part), flat(rbuf, slot))
        for m, (out, src_col, width, dst) in enumerate(pieces):
            copy = pltpu.make_async_copy(acc.at[rows, pl.ds(src_col, width)], outs[out].at[dst(n * part, part, width)],
                                         sems.at[2 + m, n])
            copy.start()
            copies.append(copy)
    for copy in copies:
        copy.wait()
    for placer in placers:
        placer.last()


def weight_grad(left, right, left_sel, right_sel, acc_shape, chunks, pieces, full_struct, carried, places, order, name):
    ranks, nb, tl = right.shape[-4], right.shape[-3], right.shape[-2]

    def at(sel, ref):
        if sel[0] == "plane":
            return (lambda step: (sel[1], slice(None), step)), ref.shape[-1]
        return (lambda step: (slice(None), step, slice(None), pl.ds(sel[1], sel[2]))), sel[2]
    left_at, left_width = at(left_sel, left)
    right_at, right_width = at(right_sel, right)
    operands, aliases = [left, right], {}
    out_shape = [full_struct, jax.ShapeDtypeStruct(acc_shape, F32)]
    scratch = [pltpu.VMEM((2, ranks, tl, left_width), BF16), pltpu.VMEM((2, ranks, tl, right_width), BF16),
               pltpu.VMEM(acc_shape, F32), pltpu.SemaphoreType.DMA((2 + len(pieces), max(2, chunks)))]
    placing = []
    for recv, full, place_pieces in places:
        src, dst = len(operands), 0
        operands.append(recv)
        if full is not None:
            dst = len(out_shape)
            aliases[len(operands)] = dst
            operands.append(full)
            out_shape.append(jax.ShapeDtypeStruct(full.shape, F32))
        placing.append((src, dst, place_pieces))
        scratch += [pltpu.VMEM((2, recv.shape[0] // nb, recv.shape[1]), F32),
                    pltpu.SemaphoreType.DMA((1 + len(place_pieces), 2))]
    if carried is not None:
        aliases[len(operands)] = 0
        operands.append(carried)
    operands += order
    rows = ranks * nb * tl
    return pl.pallas_call(
        functools.partial(weight_grad_kernel, nb, left_at, right_at, chunks, pieces, placing, len(operands), len(out_shape)),
        in_specs=[ANY] * len(operands),
        out_specs=[ANY] * len(out_shape),
        out_shape=out_shape,
        scratch_shapes=scratch,
        input_output_aliases=aliases,
        compiler_params=pltpu.CompilerParams(vmem_limit_bytes=VMEM_LIMIT),
        cost_estimate=pl.CostEstimate(flops=2 * rows * acc_shape[0] * acc_shape[1],
                                      bytes_accessed=2 * rows * (left_width + right_width) + 8 * acc_shape[0] * acc_shape[1],
                                      transcendentals=0),
        name=name,
    )(*operands)


def canonical_copies(mine_ref, pair_ref, full, sems, parts):
    core, me = my_core(), lax.axis_index('sp')
    out, src, base = [], 0, 0
    for n, width in enumerate(parts):
        for side, ref in enumerate((mine_ref.at[me], pair_ref)):
            owner = core if side == 0 else 1 - core
            dst = pl.ds(pl.multiple_of(base + owner * width, 128), width)
            out.append(pltpu.make_async_copy(ref.at[:, :, pl.ds(src, width)], full.at[:, :, dst], sems.at[n, side]))
        src += width
        base += 2 * width
    return out


def hidden_grad_kernel(parts, w_ref, x_ref, inv_ref, gain_ref, gm_ref, gp_ref, dy_ref, order_ref,
                       dx_ref, dg_ref, gfull, dn_s, xs, dys, mean_s, csem, dsem):
    del order_ref
    step = pl.program_id(0)
    steps = pl.num_programs(0)
    nb, tl, dim = dys.shape
    rows = nb * tl
    width = w_ref.shape[0]

    @pl.when(step == 0)
    def _():
        for copy in canonical_copies(gm_ref, gp_ref, gfull, csem, parts):
            copy.start()
        pltpu.make_async_copy(x_ref, xs, dsem.at[0]).start()
        pltpu.make_async_copy(dy_ref, dys, dsem.at[1]).start()
        mean_s[...] = jnp.zeros_like(mean_s)
        for copy in canonical_copies(gm_ref, gp_ref, gfull, csem, parts):
            copy.wait()

    at = lane(step, width)
    dn_s[:, at] = dot_nt(gfull[...].reshape(rows, gfull.shape[-1]), w_ref[...]).astype(BF16)

    @pl.when(step == 0)
    def _():
        pltpu.make_async_copy(x_ref, xs, dsem.at[0]).wait()

    grad = dn_s[:, at].astype(F32)
    unit = xs[:, :, at].reshape(rows, width).astype(F32) * inv_ref[...]
    prod = grad * unit
    mean_s[...] += jnp.sum(prod * gain_ref[:, at], axis=1, keepdims=True)
    dg_ref[:, at] = jnp.sum(prod, axis=0, keepdims=True)

    @pl.when(step == steps - 1)
    def _():
        pltpu.make_async_copy(dy_ref, dys, dsem.at[1]).wait()

        def finish(i, carry):
            for sub in range(tl // 16):
                here = pl.ds(sub * 16, 16)
                span = pl.ds(pl.multiple_of(i * tl + sub * 16, 16), 16)
                inv = inv_ref[span]
                unit_rows = xs[i, here].astype(F32) * inv
                inner = inv * (dn_s[span].astype(F32) * gain_ref[...] - unit_rows * (mean_s[span] * (1.0 / dim)))
                dys[i, here] = (dys[i, here].astype(F32) + inner).astype(BF16)
            pltpu.make_async_copy(dys.at[i], dx_ref.at[i], dsem.at[2]).start()
            return carry
        lax.fori_loop(0, nb, finish, 0)
        pltpu.make_async_copy(dys, dx_ref, dsem.at[2]).wait()


def hidden_grad(hidden, grad_out, inv_rms, norm_weight, w_qkv, g_all, g_pair, parts, order):
    nb, tl, dim = hidden.shape
    cols = w_qkv.shape[1]
    width = 512
    const = lambda *shape: pl.BlockSpec(shape, lambda n: (0,) * len(shape), pipeline_mode=pl.Buffered(1))
    return pl.pallas_call(
        functools.partial(hidden_grad_kernel, parts),
        grid=(dim // width,),
        in_specs=[pl.BlockSpec((width, cols), lambda n: (n, 0)), ANY, const(nb * tl, 1), const(1, dim),
                  ANY, ANY, ANY, ANY],
        out_specs=[ANY, const(1, dim)],
        out_shape=[jax.ShapeDtypeStruct((nb, tl, dim), BF16), jax.ShapeDtypeStruct((1, dim), F32)],
        scratch_shapes=[pltpu.VMEM((nb, tl, cols), BF16), pltpu.VMEM((nb * tl, dim), BF16), pltpu.VMEM((nb, tl, dim), BF16),
                        pltpu.VMEM((nb, tl, dim), BF16), pltpu.VMEM((nb * tl, 1), F32),
                        pltpu.SemaphoreType.DMA((len(parts), 2)), pltpu.SemaphoreType.DMA((3,))],
        compiler_params=pltpu.CompilerParams(dimension_semantics=("arbitrary",), vmem_limit_bytes=VMEM_LIMIT),
        cost_estimate=pl.CostEstimate(flops=2 * nb * tl * dim * cols, bytes_accessed=2 * dim * cols, transcendentals=0),
        name="hidden_grad",
    )(w_qkv, hidden, inv_rms, norm_weight, g_all, g_pair, grad_out, order)


def project_out_kernel(parts, w_ref, x_ref, om_ref, op_ref, order_ref, y_ref, ofull, csem):
    del order_ref
    nb, tl, q_dim = ofull.shape

    @pl.when(pl.program_id(0) == 0)
    def _():
        for copy in canonical_copies(om_ref, op_ref, ofull, csem, parts):
            copy.start()
        for copy in canonical_copies(om_ref, op_ref, ofull, csem, parts):
            copy.wait()

    mixed = dot_nn(ofull[...].reshape(nb * tl, q_dim), w_ref[...])
    y_ref[...] = (x_ref[...].astype(F32) + mixed.reshape(y_ref.shape)).astype(BF16)


def project_out(hidden, w_out, o_all, o_pair, parts, order):
    nb, tl, dim = hidden.shape
    q_dim = w_out.shape[0]
    width = 512
    tile = pl.BlockSpec((nb, tl, width), lambda n: (0, 0, n))
    return pl.pallas_call(
        functools.partial(project_out_kernel, parts),
        grid=(dim // width,),
        in_specs=[pl.BlockSpec((q_dim, width), lambda n: (0, n)), tile, ANY, ANY, ANY],
        out_specs=tile,
        out_shape=jax.ShapeDtypeStruct((nb, tl, dim), BF16),
        scratch_shapes=[pltpu.VMEM((nb, tl, q_dim), BF16), pltpu.SemaphoreType.DMA((len(parts), 2))],
        compiler_params=pltpu.CompilerParams(dimension_semantics=("arbitrary",), vmem_limit_bytes=VMEM_LIMIT),
        cost_estimate=pl.CostEstimate(flops=2 * nb * tl * dim * q_dim, bytes_accessed=2 * dim * q_dim, transcendentals=0),
        name="project_out",
    )(w_out, hidden, o_all, o_pair, order)


def place_kernel(steps, place_pieces, recv_ref, full_in, full_ref, bounce, tsem, psem):
    del full_in
    depth, rows = bounce.shape[0], bounce.shape[1]

    def take(n):
        return pltpu.make_async_copy(recv_ref.at[pl.ds(n * rows, rows)], bounce.at[n % depth], tsem.at[n % depth])

    def put(n):
        return [pltpu.make_async_copy(bounce.at[n % depth, :, pl.ds(col, width)], full_ref.at[dst(n * rows, rows, width)],
                                      psem.at[m, n % depth]) for m, (col, width, dst) in enumerate(place_pieces)]

    for n in range(min(depth, steps)):
        take(n).start()
    waited = 0
    for n in range(steps):
        take(n).wait()
        for copy in put(n):
            copy.start()
        if n >= depth // 2 and waited + depth < steps:
            for copy in put(waited):
                copy.wait()
            take(waited + depth).start()
            waited += 1
    for n in range(waited, steps):
        for copy in put(n):
            copy.wait()


def place(recv, full, place_pieces, steps):
    return pl.pallas_call(
        functools.partial(place_kernel, steps, place_pieces),
        in_specs=[ANY, ANY],
        out_specs=ANY,
        out_shape=jax.ShapeDtypeStruct(full.shape, F32),
        scratch_shapes=[pltpu.VMEM((8, recv.shape[0] // steps, recv.shape[1]), F32), pltpu.SemaphoreType.DMA((8,)),
                        pltpu.SemaphoreType.DMA((len(place_pieces), 8))],
        input_output_aliases={1: 0},
        compiler_params=pltpu.CompilerParams(vmem_limit_bytes=VMEM_LIMIT),
        cost_estimate=pl.CostEstimate(flops=recv.size, bytes_accessed=8 * recv.size, transcendentals=0),
        name="place",
    )(recv, full)


def group_sum_kernel(ranks, part_ref, sum_ref, parts, ssem, rsem):
    me = lax.axis_index('sp')
    barrier = pltpu.get_barrier_semaphore()
    for step in range(1, ranks):
        pl.semaphore_signal(barrier, inc=1, device_id={'sp': lax.rem(me + step, ranks)}, device_id_type=MESH)
    pl.semaphore_wait(barrier, ranks - 1)

    def copy(slot, target):
        return pltpu.make_async_remote_copy(src_ref=part_ref, dst_ref=parts.at[slot], send_sem=ssem.at[target],
                                            recv_sem=rsem.at[slot], device_id={'sp': target}, device_id_type=MESH)
    own = pltpu.make_async_copy(part_ref, parts.at[me], ssem.at[me])
    own.start()
    for step in range(1, ranks):
        copy(me, lax.rem(me + step, ranks)).start()
    own.wait()
    for step in range(1, ranks):
        rank = lax.rem(me + step, ranks)
        copy(rank, rank).wait()
    total = parts[0]
    for rank in range(1, ranks):
        total = total + parts[rank]
    sum_ref[...] = total


def group_sum(part, ranks):
    return pl.pallas_call(
        functools.partial(group_sum_kernel, ranks),
        in_specs=[ANY],
        out_specs=pl.BlockSpec(memory_space=pltpu.VMEM),
        out_shape=jax.ShapeDtypeStruct(part.shape, F32),
        scratch_shapes=[pltpu.VMEM((ranks,) + part.shape, F32), pltpu.SemaphoreType.DMA((ranks,)),
                        pltpu.SemaphoreType.DMA((ranks,))],
        compiler_params=pltpu.CompilerParams(collective_id=1, has_side_effects=True),
        cost_estimate=pl.CostEstimate(flops=ranks * part.size, bytes_accessed=8 * ranks * part.size, transcendentals=0),
        name="group_sum",
    )(part)


def block_body(ranks, hidden, positions, long_factor, norm_weight, w_qkv, w_out, grad_out):
    nb, tl, dim = hidden.shape
    hd = 2 * long_factor.shape[0]
    q_dim = w_out.shape[0]
    kv_dim = (w_qkv.shape[1] - q_dim) // 2
    pair = [(i, i ^ 1) for i in range(ranks)]
    qh, kh = q_dim // 2, kv_dim // 2

    gathered, _, inv_rms, o_all, g_all, o_send, g_send = attend(hidden, norm_weight[None], grad_out, w_qkv, w_out,
                                                                half_tables(positions, long_factor), ranks)
    o_pair = lax.ppermute(o_send, 'sp', pair)
    g_pair = lax.ppermute(g_send, 'sp', pair)

    def own_cols(base, stride):
        def where(row, rows, width):
            return (pl.ds(row, rows), pl.ds(pl.multiple_of(base + my_core() * stride, 128), width))
        return where

    def own_rows(stride):
        def where(row, rows, width):
            return (pl.ds(pl.multiple_of(my_core() * stride + row, 8), rows), pl.ds(0, width))
        return where

    def same(row, rows, width):
        return (pl.ds(row, rows), pl.ds(0, width))

    dwq_struct = jax.ShapeDtypeStruct(w_qkv.shape, F32)
    dwo_struct = jax.ShapeDtypeStruct(w_out.shape, F32)
    dwq, send_q = weight_grad(gathered, g_all, ("plane", 0), ("cols", 0, qh), (dim, qh), 8,
                              [(0, 0, qh, own_cols(0, qh)), (1, 0, qh, same)], dwq_struct, None, [], [], "wgrad_q")
    recv_q = lax.ppermute(send_q, 'sp', pair)
    dwo, send_o = weight_grad(o_all, gathered, ("cols", 0, qh), ("plane", 1), (qh, dim), 6,
                              [(0, 0, dim, own_rows(qh)), (1, 0, dim, same)], dwo_struct, None, [], [dwq, o_pair, g_pair],
                              "wgrad_out")
    recv_o = lax.ppermute(send_o, 'sp', pair)
    grad_hidden, grad_norm = hidden_grad(hidden, grad_out, inv_rms, norm_weight[None], w_qkv, g_all,
                                         g_pair, [qh, kh, kh], dwo)
    grad_norm = group_sum(grad_norm.reshape(-1, 128), ranks)
    dwq, send_kv, dwo = weight_grad(gathered, g_all, ("plane", 0), ("cols", qh, 2 * kh), (dim, 2 * kh), 8,
                                    [(0, 0, kh, own_cols(q_dim, kh)), (0, kh, kh, own_cols(q_dim + kv_dim, kh)),
                                     (1, 0, 2 * kh, same)], dwq_struct, dwq,
                                    [(recv_o, dwo, [(0, dim, peer_rows(qh))]), (recv_q, None, [(0, qh, peer_cols(0, qh))])],
                                    [grad_norm], "wgrad_kv")
    recv_kv = lax.ppermute(send_kv, 'sp', pair)
    out_hidden = project_out(hidden, w_out, o_all, o_pair, [qh], send_kv)
    dwq = place(recv_kv, dwq, [(0, kh, peer_cols(q_dim, kh)), (kh, kh, peer_cols(q_dim + kv_dim, kh))], 16)
    return out_hidden, grad_hidden, grad_norm.reshape(-1), dwq, dwo


def solution(mesh):
    token_spec = P('dp', 'sp', None)
    return jax.shard_map(functools.partial(block_body, mesh.shape['sp']), mesh=mesh,
                         in_specs=(token_spec, P(('dp', 'sp')), P(), P(), P(), P(), token_spec),
                         out_specs=(token_spec, token_spec, P('dp'), P('dp', None), P('dp', None)),
                         check_vma=False)
```
